32 devices in a mesh: lat: 2 (over core), lon: 4 (over y, x), lev: 4 (over z).
Axes of the slice: x: 2, y: 2, z: 4, core: 2. Of those that a mesh axis runs over, the one named last changes fastest.
Arguments:
- field_values: float32 [16, 512, 64, 128], P('lat', 'lon', 'lev'), may hold values from 0.2 to 1.8
- crowding: float32 [16, 512, 64, 128], P('lat', 'lon', 'lev'), may hold values from 0.5 to 2
Outputs:
- potential: float32 [16, 512, 64, 128], P('lat', 'lon', 'lev')
- field_values_end: float32 [16, 512, 64, 128], P('lat', 'lon', 'lev')
The draws below stay inside these ranges and needn't reach their ends.
All inputs are finite; a program needn't handle non-finite values.
Results may differ from the reference program's by a relative error of at most 0.00002.
Values sent between devices are 32-bit elements; how exact they have to be, the bound alone decides.
A program may use at most 256 MiB of HBM per device.

```python
import jax
import jax.numpy as jnp
from jax import lax

GRID_Y = 16
GRID_X = 512
GRID_Z = 64
LEVELS = 128
STEPS = 4


def block_levels(rng, shape, split, low, top_value):
    def one(axis_at, parts):
        heights = jax.random.uniform(jax.random.fold_in(jax.random.fold_in(rng, 6), axis_at), (parts,), jnp.float32, low / len(split), top_value / len(split))
        return jnp.repeat(jnp.exp(heights), shape[axis_at] // parts).reshape((-1,) + (1,) * (len(shape) - axis_at - 1))

    gain = one(*split[0])
    for cut in split[1:]:
        gain = gain * one(*cut)
    return gain


def setup_inputs(seed: int = 0) -> dict:
    splits = jax.random.split(jax.random.key(seed), 3)
    field_values = jnp.clip(0.2 + 1.5999999 * jax.random.uniform(splits[0], (GRID_Y, GRID_X, GRID_Z, LEVELS), jnp.float32) ** block_levels(splits[0], (GRID_Y, GRID_X, GRID_Z, LEVELS), ((0, 2), (1, 4), (2, 4)), -0.2, 0.2), 0.2, 1.8)
    crowding = jnp.clip(0.5 + 1.5 * jax.random.uniform(splits[1], (GRID_Y, GRID_X, GRID_Z, LEVELS), jnp.float32) ** block_levels(splits[1], (GRID_Y, GRID_X, GRID_Z, LEVELS), ((0, 2), (1, 4), (2, 4)), -0.2, 0.2), 0.5, 2.0)
    return {"field_values": field_values, "crowding": crowding}


def without_rim(values, dims):
    for dim in dims:
        values = lax.slice_in_dim(values, 1, values.shape[dim] - 1, axis=dim)
    return values


def shifted_cells(values, dim, start, dims):
    others = [other for other in dims if other != dim]
    values = without_rim(values, others)
    return lax.slice_in_dim(values, start, start + values.shape[dim] - 2, axis=dim)


def march_step(padded, crowding):
    middle = without_rim(padded, (0, 1, 2))
    lower = [shifted_cells(padded, dim, 0, (0, 1, 2)) for dim in (0, 1, 2)]
    upper = [shifted_cells(padded, dim, 2, (0, 1, 2)) for dim in (0, 1, 2)]
    spread = lower[0] + upper[0] + lower[1] + upper[1] + lower[2] + upper[2] - 6.0 * middle
    return middle + 0.1 * spread + 0.2 * middle * (1.0 - middle * crowding)


def reference(field_values, crowding):
    for step in range(STEPS):
        field_values = march_step(jnp.pad(field_values, ((1, 1), (1, 1), (1, 1), (0, 0)), mode="wrap"), crowding)
    potential = jnp.cumsum(field_values, axis=2) / GRID_Z
    return potential, field_values
```

```python
import functools

import jax
import jax.numpy as jnp
from jax import lax
from jax.experimental import pallas as pl
from jax.experimental.pallas import tpu as pltpu
from jax.sharding import PartitionSpec as P

STEPS = 4
BLOCK = 8
PIECES = 4
LAG = 2


def row_order(rows):
    order = []
    for k in range((rows + 1) // 2):
        order.append(k)
        if rows - 1 - k != k:
            order.append(rows - 1 - k)
    return order


def march(
    sizes, f_hbm, c_hbm, end, scan, below,
    field, crowd, lat_lo, lat_hi, lon_lo, lon_hi, lev_lo, lev_hi, face_lo, face_hi, sums,
    in_sem, face_sem, lat_send, lat_recv, lon_send, lon_recv, lev_send, lev_recv, sum_send, sum_recv,
):
    Y, X, Z, L = crowd.shape
    order = row_order(Y)
    levels_at = lax.axis_index("lev")
    last = sizes["lev"] - 1

    def beside(axis, shift):
        n = sizes[axis]
        return {axis: lax.rem(lax.axis_index(axis) + (shift + n), n)}

    def send(src, dst, send_sem, recv_sem, axis, shift):
        return pltpu.make_async_remote_copy(
            src_ref=src, dst_ref=dst, send_sem=send_sem, recv_sem=recv_sem,
            device_id=beside(axis, shift), device_id_type=pl.DeviceIdType.MESH,
        )

    def face_in(y):
        return [
            pltpu.make_async_copy(f_hbm.at[y, :, 0], face_lo.at[0, y], face_sem.at[0, y]),
            pltpu.make_async_copy(f_hbm.at[y, :, Z - 1], face_hi.at[0, y], face_sem.at[1, y]),
        ]

    f_in = [pltpu.make_async_copy(f_hbm.at[y], field.at[0, y, pl.ds(0, X)], in_sem.at[0, y]) for y in range(Y)]
    c_in = [pltpu.make_async_copy(c_hbm.at[y], crowd.at[y], in_sem.at[1, y]) for y in range(Y)]
    for y in order[:2]:
        for copy in face_in(y):
            copy.start()
    for at, y in enumerate(order):
        f_in[y].start()
        if at + 2 < Y:
            for copy in face_in(order[at + 2]):
                copy.start()
    for y in order:
        c_in[y].start()

    barrier = pltpu.get_barrier_semaphore()
    for axis in ("lev", "lat", "lon"):
        for shift in (-1, 1):
            pl.semaphore_signal(barrier, inc=1, device_id=beside(axis, shift), device_id_type=pl.DeviceIdType.MESH)
    pl.semaphore_wait(barrier, 6)

    def lev_copies(t, y):
        return [
            send(face_lo.at[t, y], lev_hi.at[t, y], lev_send.at[0, t, y], lev_recv.at[0, t, y], "lev", -1),
            send(face_hi.at[t, y], lev_lo.at[t, y], lev_send.at[1, t, y], lev_recv.at[1, t, y], "lev", 1),
        ]

    def lon_copies(t, y):
        row = field.at[t % 2, y]
        return [
            send(row.at[0], lon_hi.at[t, y], lon_send.at[0, t, y], lon_recv.at[0, t, y], "lon", -1),
            send(row.at[X - 1], lon_lo.at[t, y], lon_send.at[1, t, y], lon_recv.at[1, t, y], "lon", 1),
        ]

    def lat_low(t):
        return send(field.at[t % 2, 0, pl.ds(0, X)], lat_hi.at[t], lat_send.at[0, t], lat_recv.at[0, t], "lat", -1)

    def lat_high(t):
        return send(field.at[t % 2, Y - 1, pl.ds(0, X)], lat_lo.at[t], lat_send.at[1, t], lat_recv.at[1, t], "lat", 1)

    def send_level(t, y):
        for copy in lev_copies(t, y):
            copy.start()

    def send_plane(t, y):
        for copy in lon_copies(t, y):
            copy.start()
        if y == 0:
            lat_low(t).start()
        if y == Y - 1:
            lat_high(t).start()

    piece = X // PIECES

    def sum_copies(y):
        return [
            send(
                sums.at[y, pl.ds(p * piece, piece)], below.at[y, pl.ds(p * piece, piece)],
                sum_send.at[y, p], sum_recv.at[y, p], "lev", 1,
            )
            for p in range(PIECES)
        ]

    def pass_sums(y):
        @pl.when((levels_at > 0) & (levels_at < last))
        def _():
            for p, copy in enumerate(sum_copies(y)):
                copy.wait_recv()
                part = pl.ds(p * piece, piece)
                sums[y, part] = sums[y, part] + below[y, part]
                copy.start()

    for y in order:
        for copy in face_in(y):
            copy.wait()
        send_level(0, y)
    for y in order:
        f_in[y].wait()
        send_plane(0, y)

    @pl.when(levels_at == 0)
    def _():
        below[...] = jnp.zeros_like(below)

    place = lax.broadcasted_iota(jnp.int32, (Z, L), 0)

    for t in range(STEPS):
        now, later = t % 2, (t + 1) % 2
        if t >= 1:
            for y in order:
                for copy in lon_copies(t - 1, y):
                    copy.wait_send()
            lat_low(t - 1).wait_send()
            lat_high(t - 1).wait_send()
        for at, y in enumerate(order):
            if t == 0:
                c_in[y].wait()
            if y == 0:
                lat_high(t).wait_recv()
            if y == Y - 1:
                lat_low(t).wait_recv()
            for copy in lon_copies(t, y) + lev_copies(t, y):
                copy.wait_recv()
            before = field.at[now, y - 1] if y > 0 else lat_lo.at[t]
            after = field.at[now, y + 1] if y < Y - 1 else lat_hi.at[t]
            field[now, y, X] = lon_hi[t, y]

            def block(at, carry):
                left, middle = carry
                base = pl.multiple_of(at * BLOCK, BLOCK)
                for i in range(BLOCK):
                    x = base + i
                    right = field[now, y, x + 1]
                    lower = jnp.where(place == 0, lev_lo[t, y, pl.ds(x, 1), :], pltpu.roll(middle, 1, 0))
                    upper = jnp.where(place == Z - 1, lev_hi[t, y, pl.ds(x, 1), :], pltpu.roll(middle, Z - 1, 0))
                    around = (left + right) + (before[x] + after[x]) + (lower + upper)
                    new = 0.1 * around + middle * (0.6 - 0.2 * (middle * crowd[y, x]))
                    if t < STEPS - 1:
                        field[later, y, x] = new
                        face_lo[t + 1, y, pl.ds(x, 1), :] = new[0:1]
                        face_hi[t + 1, y, pl.ds(x, 1), :] = new[Z - 1 : Z]
                    else:
                        end[y, x] = new
                        shift = 1
                        while shift < Z:
                            new = new + jnp.where(place >= shift, pltpu.roll(new, shift, 0), 0.0)
                            shift *= 2
                        scan[y, x] = new
                        sums[y, pl.ds(x, 1), :] = new[Z - 1 : Z]
                    left, middle = middle, right
                return left, middle

            lax.fori_loop(0, X // BLOCK, block, (lon_lo[t, y], field[now, y, 0]))
            if t < STEPS - 1:
                send_level(t + 1, y)
                send_plane(t + 1, y)
            else:
                @pl.when(levels_at == 0)
                def _():
                    for copy in sum_copies(y):
                        copy.start()

                if at >= LAG:
                    pass_sums(order[at - LAG])

    for y in order[Y - LAG :]:
        pass_sums(y)

    @pl.when(levels_at == last)
    def _():
        for y in order:
            for copy in sum_copies(y):
                copy.wait_recv()

    for y in order:
        @pl.when(levels_at < last)
        def _():
            for copy in sum_copies(y):
                copy.wait_send()

        for t in range(STEPS):
            for copy in lev_copies(t, y):
                copy.wait_send()
        for copy in lon_copies(STEPS - 1, y):
            copy.wait_send()
    lat_low(STEPS - 1).wait_send()
    lat_high(STEPS - 1).wait_send()


def finish(scale, end, scan, below, pot_hbm, end_hbm, pot, out_sem):
    Y, X, Z, L = pot.shape
    ends = [pltpu.make_async_copy(end.at[y], end_hbm.at[y], out_sem.at[0, y]) for y in range(Y)]
    pots = [pltpu.make_async_copy(pot.at[y], pot_hbm.at[y], out_sem.at[1, y]) for y in range(Y)]
    for y in range(Y):
        ends[y].start()
    for y in range(Y):
        @pl.loop(0, X // BLOCK)
        def _(at):
            base = pl.multiple_of(at * BLOCK, BLOCK)
            for i in range(BLOCK):
                x = base + i
                pot[y, x] = (scan[y, x] + below[y, pl.ds(x, 1), :]) * scale

        pots[y].start()
    for y in range(Y):
        ends[y].wait()
        pots[y].wait()


def per_device(sizes, field_values, crowding):
    Y, X, Z, L = field_values.shape
    f32 = jnp.float32
    dma = pltpu.SemaphoreType.DMA
    in_hbm = pl.BlockSpec(memory_space=pltpu.HBM)
    in_vmem = pl.BlockSpec(memory_space=pltpu.VMEM)
    shape = jax.ShapeDtypeStruct(field_values.shape, f32)
    end, scan, below = pl.pallas_call(
        functools.partial(march, sizes),
        out_shape=(pltpu.VMEM((Y, X, Z, L), f32), pltpu.VMEM((Y, X, Z, L), f32), pltpu.VMEM((Y, X, L), f32)),
        in_specs=[in_hbm, in_hbm],
        out_specs=(in_vmem, in_vmem, in_vmem),
        scratch_shapes=[
            pltpu.VMEM((2, Y, X + 1, Z, L), f32),
            pltpu.VMEM((Y, X, Z, L), f32),
            pltpu.VMEM((STEPS, X, Z, L), f32),
            pltpu.VMEM((STEPS, X, Z, L), f32),
            pltpu.VMEM((STEPS, Y, Z, L), f32),
            pltpu.VMEM((STEPS, Y, Z, L), f32),
            pltpu.VMEM((STEPS, Y, X, L), f32),
            pltpu.VMEM((STEPS, Y, X, L), f32),
            pltpu.VMEM((STEPS, Y, X, L), f32),
            pltpu.VMEM((STEPS, Y, X, L), f32),
            pltpu.VMEM((Y, X, L), f32),
            dma((2, Y)),
            dma((2, Y)),
            dma((2, STEPS)),
            dma((2, STEPS)),
            dma((2, STEPS, Y)),
            dma((2, STEPS, Y)),
            dma((2, STEPS, Y)),
            dma((2, STEPS, Y)),
            dma((Y, PIECES)),
            dma((Y, PIECES)),
        ],
        compiler_params=pltpu.CompilerParams(
            collective_id=0, has_side_effects=True, vmem_limit_bytes=43 * 1024 * 1024
        ),
    )(field_values, crowding)
    return pl.pallas_call(
        functools.partial(finish, 1.0 / (Z * sizes["lev"])),
        out_shape=(shape, shape),
        in_specs=[in_vmem, in_vmem, in_vmem],
        out_specs=(in_hbm, in_hbm),
        scratch_shapes=[pltpu.VMEM((Y, X, Z, L), f32), dma((2, Y))],
        compiler_params=pltpu.CompilerParams(vmem_limit_bytes=12 * 1024 * 1024),
    )(end, scan, below)


def solution(mesh):
    return jax.shard_map(
        functools.partial(per_device, dict(mesh.shape)),
        mesh=mesh,
        in_specs=(P("lat", "lon", "lev", None), P("lat", "lon", "lev", None)),
        out_specs=(P("lat", "lon", "lev", None), P("lat", "lon", "lev", None)),
        check_vma=False,
    )
```

```python
import functools

import jax
import jax.numpy as jnp
from jax import lax
from jax.experimental import pallas as pl
from jax.experimental.pallas import tpu as pltpu
from jax.sharding import PartitionSpec as P

STEPS = 4
BLOCK = 8


def row_order(rows):
    order = []
    for k in range((rows + 1) // 2):
        order.append(k)
        if rows - 1 - k != k:
            order.append(rows - 1 - k)
    return order


def faces_first(level, rows):
    return min(1 if level == 0 else 2 + 2 * level, rows)


def last_plan(level, levels, rows):
    plan, face = [], faces_first(level, rows)
    behind = 4 * (levels - 2 - level)
    for at in range(rows):
        plan.append(("sum", at))
        if at in (2, 4) and face < rows:
            plan.append(("face", face))
            face += 1
        if level > 0 and 0 <= at - behind:
            plan.append(("top", at - behind))
    plan += [("face", at) for at in range(face, rows)]
    if level > 0:
        plan += [("top", at) for at in range(max(rows - behind, 0), rows)]
    return plan


def march(
    sizes, f_hbm, c_hbm, end, scan, base,
    field, crowd, lat, lon, lev, face, below, sums, top,
    in_sem, face_sem, lat_send, lat_recv, lon_send, lon_recv, lev_send, lev_recv, last_recv,
    top_send, top_recv, sum_send, sum_recv,
):
    Y, X, Z, L = crowd.shape
    order = row_order(Y)
    level = lax.axis_index("lev")
    levels = sizes["lev"]
    LAST = STEPS - 1
    upper_part = jnp.where(level > 0, 0.1, 0.0).astype(jnp.float32)

    def beside(axis, shift):
        n = sizes[axis]
        return {axis: lax.rem(lax.axis_index(axis) + (shift + n), n)}

    def send(src, dst, send_sem, recv_sem, axis, shift):
        return pltpu.make_async_remote_copy(
            src_ref=src, dst_ref=dst, send_sem=send_sem, recv_sem=recv_sem,
            device_id=beside(axis, shift), device_id_type=pl.DeviceIdType.MESH,
        )

    def arrived(ref, sem):
        pltpu.make_async_copy(ref, ref, sem).wait()

    def face_in(rows, group):
        return [
            pltpu.make_async_copy(f_hbm.at[rows, :, 0], face.at[0, 0, rows], face_sem.at[group, 0]),
            pltpu.make_async_copy(f_hbm.at[rows, :, Z - 1], face.at[0, 1, rows], face_sem.at[group, 1]),
        ]

    def field_in(rows, group):
        return pltpu.make_async_copy(f_hbm.at[rows], field.at[0, rows, pl.ds(0, X)], in_sem.at[group])

    inner = pl.ds(1, Y - 2)
    first_faces = face_in(pl.ds(0, 1), 0)
    other_faces = face_in(pl.ds(1, Y - 1), 1)
    f_in = [field_in(pl.ds(0, 1), 0), field_in(pl.ds(Y - 1, 1), 1), field_in(inner, 2)]
    c_in = pltpu.make_async_copy(c_hbm, crowd, in_sem.at[3])
    for copy in first_faces + other_faces + f_in:
        copy.start()
    c_in.start()

    barrier = pltpu.get_barrier_semaphore()
    for axis in ("lev", "lon", "lat"):
        for shift in (-1, 1):
            pl.semaphore_signal(barrier, inc=1, device_id=beside(axis, shift), device_id_type=pl.DeviceIdType.MESH)
    pl.semaphore_wait(barrier, 6)

    def down(t, y, sem):
        return send(face.at[t, 0, y], lev.at[t % 2, y, 1], lev_send.at[t], sem, "lev", -1)

    def up(t, y, sem):
        return send(face.at[t, 1, y], lev.at[t % 2, y, 0], lev_send.at[t], sem, "lev", 1)

    def send_level(t, y):
        up(t, y, lev_recv.at[t % 2, y]).start()
        down(t, y, lev_recv.at[t % 2, y]).start()

    def lon_copies(t, y):
        row = field.at[t % 2, y]
        s = t % 2
        return [
            send(row.at[0], lon.at[s, y, 1], lon_send.at[s], lon_recv.at[s, y], "lon", -1),
            send(row.at[X - 1], lon.at[s, y, 0], lon_send.at[s], lon_recv.at[s, y], "lon", 1),
        ]

    def send_plane(t, y):
        s = t % 2
        for copy in lon_copies(t, y):
            copy.start()
        if y == 0:
            send(field.at[s, 0, pl.ds(0, X)], lat.at[s, 1], lat_send.at[s], lat_recv.at[s], "lat", -1).start()
        if y == Y - 1:
            send(field.at[s, Y - 1, pl.ds(0, X)], lat.at[s, 0], lat_send.at[s], lat_recv.at[s], "lat", 1).start()

    def plane_sent(t):
        arrived(lon.at[t % 2], lon_send.at[t % 2])
        arrived(lat.at[t % 2], lat_send.at[t % 2])

    def rows_beside(t, y):
        before = field.at[t % 2, y - 1] if y > 0 else lat.at[t % 2, 0]
        after = field.at[t % 2, y + 1] if y < Y - 1 else lat.at[t % 2, 1]
        return before, after

    for copy in first_faces:
        copy.wait()
    send_level(0, 0)
    for copy in other_faces:
        copy.wait()
    for y in order[1:]:
        send_level(0, y)
    for copy in f_in:
        copy.wait()
    for y in order:
        send_plane(0, y)

    @pl.when(level == 0)
    def _():
        below[...] = jnp.zeros_like(below)

    c_in.wait()
    place = lax.broadcasted_iota(jnp.int32, (Z, L), 0)

    def step_row(t, y):
        now, later = t % 2, (t + 1) % 2
        if y == 0:
            arrived(lat.at[now], lat_recv.at[now])
        arrived(lon.at[now, y], lon_recv.at[now, y])
        arrived(lev.at[now, y], lev_recv.at[now, y])
        before, after = rows_beside(t, y)
        field[now, y, X] = lon[now, y, 1]

        def block(at, carry):
            left, middle = carry
            start = pl.multiple_of(at * BLOCK, BLOCK)
            for i in range(BLOCK):
                x = start + i
                right = field[now, y, x + 1]
                lower = jnp.where(place == 0, lev[now, y, 0, pl.ds(x, 1), :], pltpu.roll(middle, 1, 0))
                upper = jnp.where(place == Z - 1, lev[now, y, 1, pl.ds(x, 1), :], pltpu.roll(middle, Z - 1, 0))
                around = (left + right) + (before[x] + after[x]) + (lower + upper)
                new = 0.1 * around + middle * (0.6 - 0.2 * (middle * crowd[y, x]))
                field[later, y, x] = new
                face[t + 1, 0, y, pl.ds(x, 1), :] = new[0:1]
                face[t + 1, 1, y, pl.ds(x, 1), :] = new[Z - 1 : Z]
                left, middle = middle, right
            return left, middle

        lax.fori_loop(0, X // BLOCK, block, (lon[now, y, 0], field[now, y, 0]))

    def last_row(y):
        now = LAST % 2
        if y == 0:
            arrived(lat.at[now], lat_recv.at[now])
        arrived(lon.at[now, y], lon_recv.at[now, y])
        before, after = rows_beside(LAST, y)
        field[now, y, X] = lon[now, y, 1]

        def block(at, carry):
            left, middle = carry
            start = pl.multiple_of(at * BLOCK, BLOCK)
            for i in range(BLOCK):
                x = start + i
                right = field[now, y, x + 1]
                lower = jnp.where(place == 0, 0.0, pltpu.roll(middle, 1, 0))
                upper = jnp.where(place == Z - 1, 0.0, pltpu.roll(middle, Z - 1, 0))
                around = (left + right) + (before[x] + after[x]) + (lower + upper)
                new = 0.1 * around + middle * (0.6 - 0.2 * (middle * crowd[y, x]))
                end[y, x] = new
                shift = 1
                while shift < Z:
                    new = new + jnp.where(place >= shift, pltpu.roll(new, shift, 0), 0.0)
                    shift *= 2
                scan[y, x] = new
                sums[y, pl.ds(x, 1), :] = new[Z - 1 : Z]
                left, middle = middle, right
            return left, middle

        lax.fori_loop(0, X // BLOCK, block, (lon[now, y, 0], field[now, y, 0]))

    def sum_copy(y):
        return send(sums.at[y], below.at[y], sum_send, sum_recv.at[y], "lev", 1)

    def send_sum(y, wait):
        if wait:
            sum_copy(y).wait_recv()
        from_below = below[y] + upper_part * face[LAST, 0, y]
        sums[y] = (from_below + 0.1 * face[LAST, 1, y]) + sums[y]
        sum_copy(y).start()

    def last_down(y):
        return down(LAST, y, last_recv.at[1, y])

    def last_up(y):
        return up(LAST, y, last_recv.at[0, y])

    def send_top(y):
        send(face.at[LAST, 1, y], top.at[y], lev_send.at[LAST], top_recv.at[y], "lev", -1).start()

    def relay_top(y):
        copy = send(top.at[y], top.at[y], top_send, top_recv.at[y], "lev", -1)
        copy.wait_recv()
        copy.start()

    for t in range(LAST):
        if t >= 1:
            plane_sent(t - 1)
        for at, y in enumerate(order):
            step_row(t, y)
            if t < LAST - 1:
                send_level(t + 1, y)
            send_plane(t + 1, y)
            if t < LAST - 1:
                continue

            @pl.when(level == levels - 1)
            def _():
                send_top(y)

            @pl.when(level > 0)
            def _():
                last_down(y).start()

            for k in range(1, levels - 1):
                if at < faces_first(k, Y):
                    @pl.when(level == k)
                    def _():
                        last_up(y).start()

            if at < faces_first(0, Y):
                @pl.when(level == 0)
                def _():
                    last_down(y).start()
                    last_up(y).start()

            done = set(order[: at + 1])
            earlier = set(order[:at])
            ready = [
                row for row in order
                if {max(row - 1, 0), row, min(row + 1, Y - 1)} <= done
                and not {max(row - 1, 0), row, min(row + 1, Y - 1)} <= earlier
            ]
            for row in ready:
                last_row(row)
                place_of = order.index(row)

                @pl.when(level == 0)
                def _():
                    send_sum(row, False)
                    plan = last_plan(0, levels, Y)
                    here = plan.index(("sum", place_of))
                    for kind, which in plan[here + 1 : here + 2]:
                        if kind == "face" and place_of < Y - 1:
                            last_down(order[which]).start()
                            last_up(order[which]).start()

    @pl.when(level == 0)
    def _():
        plan = last_plan(0, levels, Y)
        left = [order[which] for kind, which in plan[plan.index(("sum", Y - 1)) + 1 :]]
        for at, y in enumerate(left):
            if at == 0:
                last_down(y).start()
            if at + 1 < len(left):
                last_down(left[at + 1]).start()
            last_up(y).start()

    for k in range(1, levels - 1):
        @pl.when(level == k)
        def _():
            for kind, which in last_plan(k, levels, Y):
                y = order[which]
                if kind == "sum":
                    send_sum(y, True)
                elif kind == "face":
                    last_up(y).start()
                else:
                    relay_top(y)

    now = LAST % 2
    for y in order:
        @pl.when(level == levels - 1)
        def _():
            sum_copy(y).wait_recv()
            top[y] = face[LAST, 1, y]

        @pl.when(level == 0)
        def _():
            arrived(top.at[y], top_recv.at[y])
            lev[now, y, 0] = top[y]

        @pl.when(level > 0)
        def _():
            last_up(y).wait_recv()

        last_down(y).wait_recv()
        base[y] = (below[y] + upper_part * face[LAST, 0, y]) + 0.1 * top[y]

        @pl.loop(0, X // BLOCK)
        def _(at):
            start = pl.multiple_of(at * BLOCK, BLOCK)
            for i in range(BLOCK):
                x = start + i
                upper = 0.1 * lev[now, y, 1, pl.ds(x, 1), :]
                end[y, x, 0:1] = end[y, x, 0:1] + 0.1 * lev[now, y, 0, pl.ds(x, 1), :]
                end[y, x, Z - 1 : Z] = end[y, x, Z - 1 : Z] + upper
                scan[y, x, Z - 1 : Z] = scan[y, x, Z - 1 : Z] + upper

    @pl.when(level < levels - 1)
    def _():
        arrived(sums, sum_send)

    @pl.when((level > 0) & (level < levels - 1))
    def _():
        arrived(top, top_send)

    for t in range(STEPS):
        arrived(face.at[t], lev_send.at[t])
    for t in (LAST - 1, LAST):
        plane_sent(t)


def finish(scale, end, scan, base, pot_hbm, end_hbm, pot, out_sem):
    Y, X, Z, L = pot.shape
    ends = [pltpu.make_async_copy(end.at[y], end_hbm.at[y], out_sem.at[0, y]) for y in range(Y)]
    pots = [pltpu.make_async_copy(pot.at[y], pot_hbm.at[y], out_sem.at[1, y]) for y in range(Y)]
    for y in range(Y):
        ends[y].start()
    for y in range(Y):
        @pl.loop(0, X // BLOCK)
        def _(at):
            start = pl.multiple_of(at * BLOCK, BLOCK)
            for i in range(BLOCK):
                x = start + i
                pot[y, x] = (scan[y, x] + base[y, pl.ds(x, 1), :]) * scale

        pots[y].start()
    for y in range(Y):
        ends[y].wait()
        pots[y].wait()


def per_device(sizes, field_values, crowding):
    Y, X, Z, L = field_values.shape
    f32 = jnp.float32
    dma = pltpu.SemaphoreType.DMA
    in_hbm = pl.BlockSpec(memory_space=pltpu.HBM)
    in_vmem = pl.BlockSpec(memory_space=pltpu.VMEM)
    shape = jax.ShapeDtypeStruct(field_values.shape, f32)
    end, scan, base = pl.pallas_call(
        functools.partial(march, sizes),
        out_shape=(pltpu.VMEM((Y, X, Z, L), f32), pltpu.VMEM((Y, X, Z, L), f32), pltpu.VMEM((Y, X, L), f32)),
        in_specs=[in_hbm, in_hbm],
        out_specs=(in_vmem, in_vmem, in_vmem),
        scratch_shapes=[
            pltpu.VMEM((2, Y, X + 1, Z, L), f32),
            pltpu.VMEM((Y, X, Z, L), f32),
            pltpu.VMEM((2, 2, X, Z, L), f32),
            pltpu.VMEM((2, Y, 2, Z, L), f32),
            pltpu.VMEM((2, Y, 2, X, L), f32),
            pltpu.VMEM((STEPS, 2, Y, X, L), f32),
            pltpu.VMEM((Y, X, L), f32),
            pltpu.VMEM((Y, X, L), f32),
            pltpu.VMEM((Y, X, L), f32),
            dma((4,)),
            dma((2, 2)),
            dma((2,)),
            dma((2,)),
            dma((2,)),
            dma((2, Y)),
            dma((STEPS,)),
            dma((2, Y)),
            dma((2, Y)),
            dma,
            dma((Y,)),
            dma,
            dma((Y,)),
        ],
        compiler_params=pltpu.CompilerParams(
            collective_id=0, has_side_effects=True, vmem_limit_bytes=40 * 1024 * 1024
        ),
    )(field_values, crowding)
    return pl.pallas_call(
        functools.partial(finish, 1.0 / (Z * sizes["lev"])),
        out_shape=(shape, shape),
        in_specs=[in_vmem, in_vmem, in_vmem],
        out_specs=(in_hbm, in_hbm),
        scratch_shapes=[pltpu.VMEM((Y, X, Z, L), f32), dma((2, Y))],
        compiler_params=pltpu.CompilerParams(vmem_limit_bytes=12 * 1024 * 1024),
    )(end, scan, base)


def solution(mesh):
    return jax.shard_map(
        functools.partial(per_device, dict(mesh.shape)),
        mesh=mesh,
        in_specs=(P("lat", "lon", "lev", None), P("lat", "lon", "lev", None)),
        out_specs=(P("lat", "lon", "lev", None), P("lat", "lon", "lev", None)),
        check_vma=False,
    )
```

```python
import functools

import jax
import jax.numpy as jnp
from jax import lax
from jax.experimental import pallas as pl
from jax.experimental.pallas import tpu as pltpu
from jax.sharding import PartitionSpec as P

STEPS = 4
BLOCK = 8


def row_order(rows):
    order = []
    for k in range((rows + 1) // 2):
        order.append(k)
        if rows - 1 - k != k:
            order.append(rows - 1 - k)
    return order


def faces_first(level, rows):
    return min(1 if level == 0 else 2 + 2 * level, rows)


def tops_before(level, levels, rows, at):
    if level == levels - 2:
        return min(at + 3, rows)
    if level == levels - 3:
        return max(min(2 * (at - 3), rows - 2), 0)
    return 0


def last_plan(level, levels, rows):
    plan, face, top = [], faces_first(level, rows), 0
    for at in range(rows):
        while level > 0 and top < tops_before(level, levels, rows, at):
            plan.append(("top", top))
            top += 1
        plan.append(("sum", at))
        if at in (2, 4) and face < rows:
            plan.append(("face", face))
            face += 1
    plan += [("face", at) for at in range(face, rows)]
    if level > 0:
        plan += [("top", at) for at in range(top, rows)]
    return plan


def march(
    sizes, f_hbm, c_hbm, end, scan, base,
    field, crowd, lat, lon, lev, face, below, sums, top,
    in_sem, face_sem, lat_send, lat_recv, lon_send, lon_recv, lev_send, lev_recv,
    top_send, top_recv, sum_send, sum_recv,
):
    Y, X, Z, L = crowd.shape
    order = row_order(Y)
    level = lax.axis_index("lev")
    levels = sizes["lev"]
    LAST = STEPS - 1
    upper_part = jnp.where(level > 0, 0.1, 0.0).astype(jnp.float32)

    def beside(axis, shift):
        n = sizes[axis]
        return {axis: lax.rem(lax.axis_index(axis) + (shift + n), n)}

    def send(src, dst, send_sem, recv_sem, axis, shift):
        return pltpu.make_async_remote_copy(
            src_ref=src, dst_ref=dst, send_sem=send_sem, recv_sem=recv_sem,
            device_id=beside(axis, shift), device_id_type=pl.DeviceIdType.MESH,
        )

    def arrived(ref, sem):
        pltpu.make_async_copy(ref, ref, sem).wait()

    def face_in(rows, group):
        return [
            pltpu.make_async_copy(f_hbm.at[rows, :, 0], face.at[0, 0, rows], face_sem.at[group, 0]),
            pltpu.make_async_copy(f_hbm.at[rows, :, Z - 1], face.at[0, 1, rows], face_sem.at[group, 1]),
        ]

    def field_in(rows, group):
        return pltpu.make_async_copy(f_hbm.at[rows], field.at[0, rows, pl.ds(0, X)], in_sem.at[group])

    inner = pl.ds(1, Y - 2)
    first_faces = face_in(pl.ds(0, 1), 0)
    other_faces = face_in(pl.ds(1, Y - 1), 1)
    f_in = [field_in(pl.ds(0, 1), 0), field_in(pl.ds(Y - 1, 1), 1), field_in(inner, 2)]
    c_in = pltpu.make_async_copy(c_hbm, crowd, in_sem.at[3])
    for copy in first_faces + other_faces + f_in:
        copy.start()
    c_in.start()

    barrier = pltpu.get_barrier_semaphore()
    for axis in ("lev", "lon", "lat"):
        for shift in (-1, 1):
            pl.semaphore_signal(barrier, inc=1, device_id=beside(axis, shift), device_id_type=pl.DeviceIdType.MESH)
    pl.semaphore_wait(barrier, 6)

    def down(t, y, sem):
        return send(face.at[t, 0, y], lev.at[t % 2, y, 1], lev_send.at[t], sem, "lev", -1)

    def up(t, y, sem):
        return send(face.at[t, 1, y], lev.at[t % 2, y, 0], lev_send.at[t], sem, "lev", 1)

    def send_level(t, y):
        up(t, y, lev_recv.at[t % 2, y]).start()
        down(t, y, lev_recv.at[t % 2, y]).start()

    def lon_copies(t, y):
        row = field.at[t % 2, y]
        s = t % 2
        return [
            send(row.at[0], lon.at[s, y, 1], lon_send.at[s], lon_recv.at[s, y], "lon", -1),
            send(row.at[X - 1], lon.at[s, y, 0], lon_send.at[s], lon_recv.at[s, y], "lon", 1),
        ]

    def send_plane(t, y):
        s = t % 2
        for copy in lon_copies(t, y):
            copy.start()
        if y == 0:
            send(field.at[s, 0, pl.ds(0, X)], lat.at[s, 1], lat_send.at[s], lat_recv.at[s], "lat", -1).start()
        if y == Y - 1:
            send(field.at[s, Y - 1, pl.ds(0, X)], lat.at[s, 0], lat_send.at[s], lat_recv.at[s], "lat", 1).start()

    def plane_sent(t):
        arrived(lon.at[t % 2], lon_send.at[t % 2])
        arrived(lat.at[t % 2], lat_send.at[t % 2])

    def rows_beside(t, y):
        before = field.at[t % 2, y - 1] if y > 0 else lat.at[t % 2, 0]
        after = field.at[t % 2, y + 1] if y < Y - 1 else lat.at[t % 2, 1]
        return before, after

    for copy in first_faces:
        copy.wait()
    send_level(0, 0)
    for copy in other_faces:
        copy.wait()
    for y in order[1:]:
        send_level(0, y)
    for copy in f_in:
        copy.wait()
    for y in order:
        send_plane(0, y)

    @pl.when(level == 0)
    def _():
        below[...] = jnp.zeros_like(below)

    c_in.wait()
    place = lax.broadcasted_iota(jnp.int32, (Z, L), 0)

    def step_row(t, y):
        now, later = t % 2, (t + 1) % 2
        if y == 0:
            arrived(lat.at[now], lat_recv.at[now])
        arrived(lon.at[now, y], lon_recv.at[now, y])
        arrived(lev.at[now, y], lev_recv.at[now, y])
        before, after = rows_beside(t, y)
        field[now, y, X] = lon[now, y, 1]

        def block(at, carry):
            left, middle = carry
            start = pl.multiple_of(at * BLOCK, BLOCK)
            for i in range(BLOCK):
                x = start + i
                right = field[now, y, x + 1]
                lower = jnp.where(place == 0, lev[now, y, 0, pl.ds(x, 1), :], pltpu.roll(middle, 1, 0))
                upper = jnp.where(place == Z - 1, lev[now, y, 1, pl.ds(x, 1), :], pltpu.roll(middle, Z - 1, 0))
                around = (left + right) + (before[x] + after[x]) + (lower + upper)
                new = 0.1 * around + middle * (0.6 - 0.2 * (middle * crowd[y, x]))
                field[later, y, x] = new
                face[t + 1, 0, y, pl.ds(x, 1), :] = new[0:1]
                face[t + 1, 1, y, pl.ds(x, 1), :] = new[Z - 1 : Z]
                left, middle = middle, right
            return left, middle

        lax.fori_loop(0, X // BLOCK, block, (lon[now, y, 0], field[now, y, 0]))

    def last_row(y):
        now = LAST % 2
        if y == 0:
            arrived(lat.at[now], lat_recv.at[now])
        arrived(lon.at[now, y], lon_recv.at[now, y])
        before, after = rows_beside(LAST, y)
        field[now, y, X] = lon[now, y, 1]

        def block(at, carry):
            left, middle = carry
            start = pl.multiple_of(at * BLOCK, BLOCK)
            for i in range(BLOCK):
                x = start + i
                right = field[now, y, x + 1]
                lower = jnp.where(place == 0, 0.0, pltpu.roll(middle, 1, 0))
                upper = jnp.where(place == Z - 1, 0.0, pltpu.roll(middle, Z - 1, 0))
                around = (left + right) + (before[x] + after[x]) + (lower + upper)
                new = 0.1 * around + middle * (0.6 - 0.2 * (middle * crowd[y, x]))
                end[y, x] = new
                shift = 1
                while shift < Z:
                    new = new + jnp.where(place >= shift, pltpu.roll(new, shift, 0), 0.0)
                    shift *= 2
                scan[y, x] = new
                sums[y, pl.ds(x, 1), :] = new[Z - 1 : Z]
                left, middle = middle, right
            return left, middle

        lax.fori_loop(0, X // BLOCK, block, (lon[now, y, 0], field[now, y, 0]))

    def sum_copy(y):
        return send(sums.at[y], below.at[y], sum_send, sum_recv.at[y], "lev", 1)

    def send_sum(y, wait):
        if wait:
            sum_copy(y).wait_recv()
        from_below = below[y] + upper_part * face[LAST, 0, y]
        sums[y] = (from_below + 0.1 * face[LAST, 1, y]) + sums[y]
        sum_copy(y).start()

    def last_down(y):
        return down(LAST, y, lev_recv.at[LAST % 2, y])

    def last_up(y):
        return up(LAST, y, lev_recv.at[LAST % 2, y])

    def send_top(y):
        send(face.at[LAST, 1, y], top.at[y], lev_send.at[LAST], top_recv.at[y], "lev", -1).start()

    def relay_top(y):
        copy = send(top.at[y], top.at[y], top_send, top_recv.at[y], "lev", -1)
        copy.wait_recv()
        copy.start()

    for t in range(LAST):
        if t >= 1:
            plane_sent(t - 1)
        for at, y in enumerate(order):
            step_row(t, y)
            if t < LAST - 1:
                send_level(t + 1, y)
            send_plane(t + 1, y)
            if t < LAST - 1:
                continue

            @pl.when(level == levels - 1)
            def _():
                send_top(y)

            @pl.when(level > 0)
            def _():
                last_down(y).start()

            for k in range(1, levels - 1):
                if at < faces_first(k, Y):
                    @pl.when(level == k)
                    def _():
                        last_up(y).start()

            if at < faces_first(0, Y):
                @pl.when(level == 0)
                def _():
                    last_down(y).start()
                    last_up(y).start()

            done = set(order[: at + 1])
            earlier = set(order[:at])
            ready = [
                row for row in order
                if {max(row - 1, 0), row, min(row + 1, Y - 1)} <= done
                and not {max(row - 1, 0), row, min(row + 1, Y - 1)} <= earlier
            ]
            for row in ready:
                last_row(row)
                place_of = order.index(row)

                @pl.when(level == 0)
                def _():
                    send_sum(row, False)
                    plan = last_plan(0, levels, Y)
                    here = plan.index(("sum", place_of))
                    for kind, which in plan[here + 1 : here + 2]:
                        if kind == "face" and place_of < Y - 1:
                            last_down(order[which]).start()
                            last_up(order[which]).start()

    @pl.when(level == 0)
    def _():
        plan = last_plan(0, levels, Y)
        left = [order[which] for kind, which in plan[plan.index(("sum", Y - 1)) + 1 :]]
        for at, y in enumerate(left):
            if at == 0:
                last_down(y).start()
            if at + 1 < len(left):
                last_down(left[at + 1]).start()
            last_up(y).start()

    for k in range(1, levels - 1):
        @pl.when(level == k)
        def _():
            for kind, which in last_plan(k, levels, Y):
                y = order[which]
                if kind == "sum":
                    send_sum(y, True)
                elif kind == "face":
                    last_up(y).start()
                else:
                    relay_top(y)

    now = LAST % 2
    for y in order:
        @pl.when(level == levels - 1)
        def _():
            sum_copy(y).wait_recv()
            top[y] = face[LAST, 1, y]

        @pl.when(level == 0)
        def _():
            arrived(top.at[y], top_recv.at[y])
            lev[now, y, 0] = top[y]
            last_down(y).wait_recv()

        @pl.when(level > 0)
        def _():
            arrived(lev.at[now, y], lev_recv.at[now, y])

        base[y] = (below[y] + upper_part * face[LAST, 0, y]) + 0.1 * top[y]

        @pl.loop(0, X // BLOCK)
        def _(at):
            some = pl.ds(pl.multiple_of(at * BLOCK, BLOCK), BLOCK)
            upper = 0.1 * lev[now, y, 1, some, :]
            end[y, some, 0, :] = end[y, some, 0, :] + 0.1 * lev[now, y, 0, some, :]
            end[y, some, Z - 1, :] = end[y, some, Z - 1, :] + upper
            scan[y, some, Z - 1, :] = scan[y, some, Z - 1, :] + upper

    @pl.when(level < levels - 1)
    def _():
        arrived(sums, sum_send)

    @pl.when((level > 0) & (level < levels - 1))
    def _():
        arrived(top, top_send)

    for t in range(STEPS):
        arrived(face.at[t], lev_send.at[t])
    for t in (LAST - 1, LAST):
        plane_sent(t)


def finish(scale, end, scan, base, pot_hbm, end_hbm, pot, out_sem):
    Y, X, Z, L = pot.shape
    ends = pltpu.make_async_copy(end, end_hbm, out_sem.at[0])
    ends.start()
    for y in range(Y):
        @pl.loop(0, X // BLOCK)
        def _(at):
            start = pl.multiple_of(at * BLOCK, BLOCK)
            for i in range(BLOCK):
                x = start + i
                pot[y, x] = (scan[y, x] + base[y, pl.ds(x, 1), :]) * scale

        pltpu.make_async_copy(pot.at[y], pot_hbm.at[y], out_sem.at[1]).start()
    ends.wait()
    pltpu.make_async_copy(pot, pot_hbm, out_sem.at[1]).wait()


def per_device(sizes, field_values, crowding):
    Y, X, Z, L = field_values.shape
    f32 = jnp.float32
    dma = pltpu.SemaphoreType.DMA
    in_hbm = pl.BlockSpec(memory_space=pltpu.HBM)
    in_vmem = pl.BlockSpec(memory_space=pltpu.VMEM)
    shape = jax.ShapeDtypeStruct(field_values.shape, f32)
    end, scan, base = pl.pallas_call(
        functools.partial(march, sizes),
        out_shape=(pltpu.VMEM((Y, X, Z, L), f32), pltpu.VMEM((Y, X, Z, L), f32), pltpu.VMEM((Y, X, L), f32)),
        in_specs=[in_hbm, in_hbm],
        out_specs=(in_vmem, in_vmem, in_vmem),
        scratch_shapes=[
            pltpu.VMEM((2, Y, X + 1, Z, L), f32),
            pltpu.VMEM((Y, X, Z, L), f32),
            pltpu.VMEM((2, 2, X, Z, L), f32),
            pltpu.VMEM((2, Y, 2, Z, L), f32),
            pltpu.VMEM((2, Y, 2, X, L), f32),
            pltpu.VMEM((STEPS, 2, Y, X, L), f32),
            pltpu.VMEM((Y, X, L), f32),
            pltpu.VMEM((Y, X, L), f32),
            pltpu.VMEM((Y, X, L), f32),
            dma((4,)),
            dma((2, 2)),
            dma((2,)),
            dma((2,)),
            dma((2,)),
            dma((2, Y)),
            dma((STEPS,)),
            dma((2, Y)),
            dma,
            dma((Y,)),
            dma,
            dma((Y,)),
        ],
        compiler_params=pltpu.CompilerParams(
            collective_id=0, has_side_effects=True, vmem_limit_bytes=40 * 1024 * 1024
        ),
    )(field_values, crowding)
    return pl.pallas_call(
        functools.partial(finish, 1.0 / (Z * sizes["lev"])),
        out_shape=(shape, shape),
        in_specs=[in_vmem, in_vmem, in_vmem],
        out_specs=(in_hbm, in_hbm),
        scratch_shapes=[pltpu.VMEM((Y, X, Z, L), f32), dma((2,))],
        compiler_params=pltpu.CompilerParams(vmem_limit_bytes=12 * 1024 * 1024),
    )(end, scan, base)


def solution(mesh):
    return jax.shard_map(
        functools.partial(per_device, dict(mesh.shape)),
        mesh=mesh,
        in_specs=(P("lat", "lon", "lev", None), P("lat", "lon", "lev", None)),
        out_specs=(P("lat", "lon", "lev", None), P("lat", "lon", "lev", None)),
        check_vma=False,
    )
```

```python
import functools

import jax
import jax.numpy as jnp
from jax import lax
from jax.experimental import pallas as pl
from jax.experimental.pallas import tpu as pltpu
from jax.sharding import PartitionSpec as P

STEPS = 4
BLOCK = 8
PIECE = 64


def row_order(rows):
    order = []
    for k in range((rows + 1) // 2):
        order.append(k)
        if rows - 1 - k != k:
            order.append(rows - 1 - k)
    return order


def faces_first(level, rows):
    return min(1 if level == 0 else 2 + 2 * level, rows)


def tops_before(level, levels, rows, at):
    if level == levels - 2:
        return min(at + 3, rows)
    if level == levels - 3:
        return max(min(2 * (at - 3), rows - 2), 0)
    return 0


def last_plan(level, levels, rows):
    plan, face, top = [], faces_first(level, rows), 0
    for at in range(rows):
        while level > 0 and top < tops_before(level, levels, rows, at):
            plan.append(("top", top))
            top += 1
        plan.append(("sum", at))
        if at in (2, 4) and face < rows:
            plan.append(("face", face))
            face += 1
    plan += [("face", at) for at in range(face, rows)]
    if level > 0:
        plan += [("top", at) for at in range(top, rows)]
    return plan


def march(
    sizes, f_hbm, c_hbm, end, scan, base,
    field, crowd, lat, lon, lev, face, below, sums, top,
    in_sem, face_sem, lat_send, lat_recv, lon_send, lon_recv, lev_send, lev_recv,
    top_send, top_recv, sum_send, sum_recv, ends_sem,
):
    Y, X, Z, L = crowd.shape
    order = row_order(Y)
    level = lax.axis_index("lev")
    levels = sizes["lev"]
    LAST = STEPS - 1
    upper_part = jnp.where(level > 0, 0.1, 0.0).astype(jnp.float32)

    def beside(axis, shift):
        n = sizes[axis]
        return {axis: lax.rem(lax.axis_index(axis) + (shift + n), n)}

    def send(src, dst, send_sem, recv_sem, axis, shift):
        return pltpu.make_async_remote_copy(
            src_ref=src, dst_ref=dst, send_sem=send_sem, recv_sem=recv_sem,
            device_id=beside(axis, shift), device_id_type=pl.DeviceIdType.MESH,
        )

    def arrived(ref, sem):
        pltpu.make_async_copy(ref, ref, sem).wait()

    def face_in(rows, group):
        return [
            pltpu.make_async_copy(f_hbm.at[rows, :, 0], face.at[0, 0, rows], face_sem.at[group, 0]),
            pltpu.make_async_copy(f_hbm.at[rows, :, Z - 1], face.at[0, 1, rows], face_sem.at[group, 1]),
        ]

    def field_in(rows, group):
        return pltpu.make_async_copy(f_hbm.at[rows], field.at[0, rows, pl.ds(0, X)], in_sem.at[group])

    inner = pl.ds(1, Y - 2)
    first_faces = face_in(pl.ds(0, 1), 0)
    other_faces = face_in(pl.ds(1, Y - 1), 1)
    f_in = [field_in(pl.ds(0, 1), 0), field_in(pl.ds(Y - 1, 1), 1), field_in(inner, 2)]
    c_in = pltpu.make_async_copy(c_hbm, crowd, in_sem.at[3])
    for copy in first_faces + other_faces + f_in:
        copy.start()
    c_in.start()

    places = {axis: lax.axis_index(axis) for axis in ("lev", "lon")}
    barrier = pltpu.get_barrier_semaphore()

    def signal(sem, axis, shift):
        pl.semaphore_signal(sem, inc=1, device_id=beside(axis, shift), device_id_type=pl.DeviceIdType.MESH)

    greeted = 1
    for axis, place in places.items():
        @pl.when(place > 0)
        def _():
            signal(barrier, axis, -1)

        @pl.when(place < sizes[axis] - 1)
        def _():
            signal(barrier, axis, 1)

        greeted += jnp.where(place > 0, 1, 0) + jnp.where(place < sizes[axis] - 1, 1, 0)
    signal(barrier, "lat", 1)
    pl.semaphore_wait(barrier, greeted)

    for at, (axis, place) in enumerate(places.items()):
        @pl.when(place == 0)
        def _():
            signal(ends_sem.at[at, 0], axis, 1)

        @pl.when(place == sizes[axis] - 1)
        def _():
            signal(ends_sem.at[at, 1], axis, -1)

    def meet_ends(axis):
        at, place = list(places).index(axis), places[axis]

        @pl.when(place > 0)
        def _():
            pl.semaphore_wait(ends_sem.at[at, 0], 1)

            @pl.when(place < sizes[axis] - 1)
            def _():
                signal(ends_sem.at[at, 0], axis, 1)

        @pl.when(place < sizes[axis] - 1)
        def _():
            pl.semaphore_wait(ends_sem.at[at, 1], 1)

            @pl.when(place > 0)
            def _():
                signal(ends_sem.at[at, 1], axis, -1)

    def down(t, y, sem):
        return send(face.at[t, 0, y], lev.at[t % 2, y, 1], lev_send.at[t], sem, "lev", -1)

    def up(t, y, sem):
        return send(face.at[t, 1, y], lev.at[t % 2, y, 0], lev_send.at[t], sem, "lev", 1)

    def send_level(t, y):
        up(t, y, lev_recv.at[t % 2, y]).start()
        down(t, y, lev_recv.at[t % 2, y]).start()

    def lon_copies(t, y):
        row = field.at[t % 2, y]
        s = t % 2
        return [
            send(row.at[0], lon.at[s, y, 1], lon_send.at[s], lon_recv.at[s, y], "lon", -1),
            send(row.at[X - 1], lon.at[s, y, 0], lon_send.at[s], lon_recv.at[s, y], "lon", 1),
        ]

    def send_plane(t, y):
        s = t % 2
        for copy in lon_copies(t, y):
            copy.start()
        if y == 0:
            send(field.at[s, 0, pl.ds(0, X)], lat.at[s, 1], lat_send.at[s], lat_recv.at[s], "lat", -1).start()
        if y == Y - 1:
            send(field.at[s, Y - 1, pl.ds(0, X)], lat.at[s, 0], lat_send.at[s], lat_recv.at[s], "lat", 1).start()

    def plane_sent(t):
        arrived(lon.at[t % 2], lon_send.at[t % 2])
        arrived(lat.at[t % 2], lat_send.at[t % 2])

    def rows_beside(t, y):
        before = field.at[t % 2, y - 1] if y > 0 else lat.at[t % 2, 0]
        after = field.at[t % 2, y + 1] if y < Y - 1 else lat.at[t % 2, 1]
        return before, after

    def start_level(y, wrap):
        @pl.when((level == levels - 1) if wrap else (level < levels - 1))
        def _():
            up(0, y, lev_recv.at[0, y]).start()

        @pl.when((level == 0) if wrap else (level > 0))
        def _():
            down(0, y, lev_recv.at[0, y]).start()

    for copy in first_faces:
        copy.wait()
    start_level(0, False)
    for copy in other_faces:
        copy.wait()
    ahead = Y // 2
    for y in order[1:ahead]:
        start_level(y, False)

    @pl.when((level > 0) & (level < levels - 1))
    def _():
        for y in order[ahead:]:
            start_level(y, False)

    meet_ends("lev")

    @pl.when((level == 0) | (level == levels - 1))
    def _():
        for y in order[:ahead]:
            start_level(y, True)
        for y in order[ahead:]:
            start_level(y, False)
            start_level(y, True)

    for copy in f_in:
        copy.wait()
    meet_ends("lon")
    for y in order:
        send_plane(0, y)

    @pl.when(level == 0)
    def _():
        below[...] = jnp.zeros_like(below)

    c_in.wait()
    place = lax.broadcasted_iota(jnp.int32, (Z, L), 0)

    def step_row(t, y):
        now, later = t % 2, (t + 1) % 2
        if y == 0:
            arrived(lat.at[now], lat_recv.at[now])
        arrived(lon.at[now, y], lon_recv.at[now, y])
        arrived(lev.at[now, y], lev_recv.at[now, y])
        before, after = rows_beside(t, y)
        field[now, y, X] = lon[now, y, 1]

        def block(at, carry):
            left, middle = carry
            start = pl.multiple_of(at * BLOCK, BLOCK)
            for i in range(BLOCK):
                x = start + i
                right = field[now, y, x + 1]
                lower = jnp.where(place == 0, lev[now, y, 0, pl.ds(x, 1), :], pltpu.roll(middle, 1, 0))
                upper = jnp.where(place == Z - 1, lev[now, y, 1, pl.ds(x, 1), :], pltpu.roll(middle, Z - 1, 0))
                around = (left + right) + (before[x] + after[x]) + (lower + upper)
                new = 0.1 * around + middle * (0.6 - 0.2 * (middle * crowd[y, x]))
                field[later, y, x] = new
                face[t + 1, 0, y, pl.ds(x, 1), :] = new[0:1]
                face[t + 1, 1, y, pl.ds(x, 1), :] = new[Z - 1 : Z]
                left, middle = middle, right
            return left, middle

        lax.fori_loop(0, X // BLOCK, block, (lon[now, y, 0], field[now, y, 0]))

    def last_row(y):
        now = LAST % 2
        if y == 0:
            arrived(lat.at[now], lat_recv.at[now])
        arrived(lon.at[now, y], lon_recv.at[now, y])
        before, after = rows_beside(LAST, y)
        field[now, y, X] = lon[now, y, 1]

        def block(at, carry):
            left, middle = carry
            start = pl.multiple_of(at * BLOCK, BLOCK)
            for i in range(BLOCK):
                x = start + i
                right = field[now, y, x + 1]
                lower = jnp.where(place == 0, 0.0, pltpu.roll(middle, 1, 0))
                upper = jnp.where(place == Z - 1, 0.0, pltpu.roll(middle, Z - 1, 0))
                around = (left + right) + (before[x] + after[x]) + (lower + upper)
                new = 0.1 * around + middle * (0.6 - 0.2 * (middle * crowd[y, x]))
                end[y, x] = new
                shift = 1
                while shift < Z:
                    new = new + jnp.where(place >= shift, pltpu.roll(new, shift, 0), 0.0)
                    shift *= 2
                scan[y, x] = new
                sums[y, pl.ds(x, 1), :] = new[Z - 1 : Z]
                left, middle = middle, right
            return left, middle

        lax.fori_loop(0, X // BLOCK, block, (lon[now, y, 0], field[now, y, 0]))

    def sum_copy(y):
        return send(sums.at[y], below.at[y], sum_send, sum_recv.at[y], "lev", 1)

    def send_sum(y, wait):
        if wait:
            sum_copy(y).wait_recv()
        from_below = below[y] + upper_part * face[LAST, 0, y]
        sums[y] = (from_below + 0.1 * face[LAST, 1, y]) + sums[y]
        sum_copy(y).start()

    def last_down(y):
        return down(LAST, y, lev_recv.at[LAST % 2, y])

    def last_up(y):
        return up(LAST, y, lev_recv.at[LAST % 2, y])

    def send_top(y):
        send(face.at[LAST, 1, y], top.at[y], lev_send.at[LAST], top_recv.at[y], "lev", -1).start()

    def relay_top(y):
        copy = send(top.at[y], top.at[y], top_send, top_recv.at[y], "lev", -1)
        copy.wait_recv()
        copy.start()

    for t in range(LAST):
        if t >= 1:
            plane_sent(t - 1)
        for at, y in enumerate(order):
            step_row(t, y)
            if t < LAST - 1:
                send_level(t + 1, y)
            send_plane(t + 1, y)
            if t < LAST - 1:
                continue

            @pl.when(level == levels - 1)
            def _():
                send_top(y)

            @pl.when(level > 0)
            def _():
                last_down(y).start()

            for k in range(1, levels - 1):
                if at < faces_first(k, Y):
                    @pl.when(level == k)
                    def _():
                        last_up(y).start()

            if at < faces_first(0, Y):
                @pl.when(level == 0)
                def _():
                    last_down(y).start()
                    last_up(y).start()

            done = set(order[: at + 1])
            earlier = set(order[:at])
            ready = [
                row for row in order
                if {max(row - 1, 0), row, min(row + 1, Y - 1)} <= done
                and not {max(row - 1, 0), row, min(row + 1, Y - 1)} <= earlier
            ]
            for row in ready:
                last_row(row)
                place_of = order.index(row)

                @pl.when(level == 0)
                def _():
                    send_sum(row, False)
                    plan = last_plan(0, levels, Y)
                    here = plan.index(("sum", place_of))
                    for kind, which in plan[here + 1 : here + 2]:
                        if kind == "face" and place_of < Y - 1:
                            last_down(order[which]).start()
                            last_up(order[which]).start()

    @pl.when(level == 0)
    def _():
        plan = last_plan(0, levels, Y)
        left = [order[which] for kind, which in plan[plan.index(("sum", Y - 1)) + 1 :]]
        for at, y in enumerate(left):
            if at == 0:
                last_down(y).start()
            if at + 1 < len(left):
                last_down(left[at + 1]).start()
            last_up(y).start()

    for k in range(1, levels - 1):
        @pl.when(level == k)
        def _():
            for kind, which in last_plan(k, levels, Y):
                y = order[which]
                if kind == "sum":
                    send_sum(y, True)
                elif kind == "face":
                    last_up(y).start()
                else:
                    relay_top(y)

    now = LAST % 2
    for y in order:
        @pl.when(level == levels - 1)
        def _():
            sum_copy(y).wait_recv()
            top[y] = face[LAST, 1, y]

        @pl.when(level == 0)
        def _():
            arrived(top.at[y], top_recv.at[y])
            lev[now, y, 0] = top[y]
            last_down(y).wait_recv()

        @pl.when(level > 0)
        def _():
            arrived(lev.at[now, y], lev_recv.at[now, y])

        base[y] = (below[y] + upper_part * face[LAST, 0, y]) + 0.1 * top[y]

        for start in range(0, X, PIECE):
            some = pl.ds(start, PIECE)
            upper = 0.1 * lev[now, y, 1, some, :]
            end[y, some, 0, :] = end[y, some, 0, :] + 0.1 * lev[now, y, 0, some, :]
            end[y, some, Z - 1, :] = end[y, some, Z - 1, :] + upper
            scan[y, some, Z - 1, :] = scan[y, some, Z - 1, :] + upper

    @pl.when(level < levels - 1)
    def _():
        arrived(sums, sum_send)

    @pl.when((level > 0) & (level < levels - 1))
    def _():
        arrived(top, top_send)

    for t in range(STEPS):
        arrived(face.at[t], lev_send.at[t])
    for t in (LAST - 1, LAST):
        plane_sent(t)


def finish(scale, end, scan, base, pot_hbm, end_hbm, pot, out_sem):
    Y, X, Z, L = pot.shape
    ends = pltpu.make_async_copy(end, end_hbm, out_sem.at[0])
    ends.start()
    for y in range(Y):
        @pl.loop(0, X // BLOCK)
        def _(at):
            start = pl.multiple_of(at * BLOCK, BLOCK)
            for i in range(BLOCK):
                x = start + i
                pot[y, x] = (scan[y, x] + base[y, pl.ds(x, 1), :]) * scale

        pltpu.make_async_copy(pot.at[y], pot_hbm.at[y], out_sem.at[1]).start()
    ends.wait()
    pltpu.make_async_copy(pot, pot_hbm, out_sem.at[1]).wait()


def per_device(sizes, field_values, crowding):
    Y, X, Z, L = field_values.shape
    f32 = jnp.float32
    dma = pltpu.SemaphoreType.DMA
    in_hbm = pl.BlockSpec(memory_space=pltpu.HBM)
    in_vmem = pl.BlockSpec(memory_space=pltpu.VMEM)
    shape = jax.ShapeDtypeStruct(field_values.shape, f32)
    end, scan, base = pl.pallas_call(
        functools.partial(march, sizes),
        out_shape=(pltpu.VMEM((Y, X, Z, L), f32), pltpu.VMEM((Y, X, Z, L), f32), pltpu.VMEM((Y, X, L), f32)),
        in_specs=[in_hbm, in_hbm],
        out_specs=(in_vmem, in_vmem, in_vmem),
        scratch_shapes=[
            pltpu.VMEM((2, Y, X + 1, Z, L), f32),
            pltpu.VMEM((Y, X, Z, L), f32),
            pltpu.VMEM((2, 2, X, Z, L), f32),
            pltpu.VMEM((2, Y, 2, Z, L), f32),
            pltpu.VMEM((2, Y, 2, X, L), f32),
            pltpu.VMEM((STEPS, 2, Y, X, L), f32),
            pltpu.VMEM((Y, X, L), f32),
            pltpu.VMEM((Y, X, L), f32),
            pltpu.VMEM((Y, X, L), f32),
            dma((4,)),
            dma((2, 2)),
            dma((2,)),
            dma((2,)),
            dma((2,)),
            dma((2, Y)),
            dma((STEPS,)),
            dma((2, Y)),
            dma,
            dma((Y,)),
            dma,
            dma((Y,)),
            pltpu.SemaphoreType.REGULAR((2, 2)),
        ],
        compiler_params=pltpu.CompilerParams(
            collective_id=0, has_side_effects=True, vmem_limit_bytes=40 * 1024 * 1024
        ),
    )(field_values, crowding)
    return pl.pallas_call(
        functools.partial(finish, 1.0 / (Z * sizes["lev"])),
        out_shape=(shape, shape),
        in_specs=[in_vmem, in_vmem, in_vmem],
        out_specs=(in_hbm, in_hbm),
        scratch_shapes=[pltpu.VMEM((Y, X, Z, L), f32), dma((2,))],
        compiler_params=pltpu.CompilerParams(vmem_limit_bytes=12 * 1024 * 1024),
    )(end, scan, base)


def solution(mesh):
    return jax.shard_map(
        functools.partial(per_device, dict(mesh.shape)),
        mesh=mesh,
        in_specs=(P("lat", "lon", "lev", None), P("lat", "lon", "lev", None)),
        out_specs=(P("lat", "lon", "lev", None), P("lat", "lon", "lev", None)),
        check_vma=False,
    )
```

```python
import functools

import jax
import jax.numpy as jnp
from jax import lax
from jax.experimental import pallas as pl
from jax.experimental.pallas import tpu as pltpu
from jax.sharding import PartitionSpec as P

STEPS = 4
BLOCK = 8
PIECE = 64


def row_order(rows):
    order = []
    for k in range((rows + 1) // 2):
        order.append(k)
        if rows - 1 - k != k:
            order.append(rows - 1 - k)
    return order


def faces_first(level, rows):
    return min(2 + 2 * level, rows)


def tops_before(level, levels, rows, at):
    if level == levels - 2:
        return min(at + 3, rows)
    if level == levels - 3:
        return max(min(2 * (at - 3), rows - 2), 0)
    return 0


def last_plan(level, levels, rows):
    plan, top = [], 0
    for at in range(rows):
        while top < tops_before(level, levels, rows, at):
            plan.append(("top", top))
            top += 1
        plan.append(("sum", at))
    plan += [("face", at) for at in range(faces_first(level, rows), rows)]
    plan += [("top", at) for at in range(top, rows)]
    return plan


def march(
    sizes, f_hbm, c_hbm, end, scan, base,
    field, crowd, lat, lon, lev, face, below, sums, top,
    in_sem, face_sem, lat_send, lat_recv, lon_send, lon_recv, lev_send, lev_recv,
    top_send, top_recv, sum_send, sum_recv, ends_sem,
):
    Y, X, Z, L = crowd.shape
    order = row_order(Y)
    level = lax.axis_index("lev")
    levels = sizes["lev"]
    LAST = STEPS - 1
    upper_part = jnp.where(level > 0, 0.1, 0.0).astype(jnp.float32)

    def beside(axis, shift):
        n = sizes[axis]
        return {axis: lax.rem(lax.axis_index(axis) + (shift + n), n)}

    def send(src, dst, send_sem, recv_sem, axis, shift):
        return pltpu.make_async_remote_copy(
            src_ref=src, dst_ref=dst, send_sem=send_sem, recv_sem=recv_sem,
            device_id=beside(axis, shift), device_id_type=pl.DeviceIdType.MESH,
        )

    def arrived(ref, sem):
        pltpu.make_async_copy(ref, ref, sem).wait()

    def face_in(rows, group):
        return [
            pltpu.make_async_copy(f_hbm.at[rows, :, 0], face.at[0, 0, rows], face_sem.at[group, 0]),
            pltpu.make_async_copy(f_hbm.at[rows, :, Z - 1], face.at[0, 1, rows], face_sem.at[group, 1]),
        ]

    def field_in(rows, group):
        return pltpu.make_async_copy(f_hbm.at[rows], field.at[0, rows, pl.ds(0, X)], in_sem.at[group])

    inner = pl.ds(1, Y - 2)
    faces_in = [face_in(pl.ds(0, 1), 0), face_in(pl.ds(Y - 1, 1), 1), face_in(inner, 2)]
    f_in = [field_in(pl.ds(0, 1), 0), field_in(pl.ds(Y - 1, 1), 1), field_in(inner, 2)]
    c_in = pltpu.make_async_copy(c_hbm, crowd, in_sem.at[3])
    for copy in faces_in[0] + faces_in[1] + faces_in[2] + f_in:
        copy.start()
    c_in.start()

    places = {axis: lax.axis_index(axis) for axis in ("lev", "lon")}
    barrier = pltpu.get_barrier_semaphore()

    def signal(sem, axis, shift):
        pl.semaphore_signal(sem, inc=1, device_id=beside(axis, shift), device_id_type=pl.DeviceIdType.MESH)

    greeted = 1
    for axis, place in places.items():
        @pl.when(place > 0)
        def _():
            signal(barrier, axis, -1)

        @pl.when(place < sizes[axis] - 1)
        def _():
            signal(barrier, axis, 1)

        greeted += jnp.where(place > 0, 1, 0) + jnp.where(place < sizes[axis] - 1, 1, 0)
    signal(barrier, "lat", 1)
    pl.semaphore_wait(barrier, greeted)

    for at, (axis, place) in enumerate(places.items()):
        @pl.when(place == 0)
        def _():
            signal(ends_sem.at[at, 0], axis, 1)

        @pl.when(place == sizes[axis] - 1)
        def _():
            signal(ends_sem.at[at, 1], axis, -1)

    def meet_ends(axis):
        at, place = list(places).index(axis), places[axis]

        @pl.when(place > 0)
        def _():
            pl.semaphore_wait(ends_sem.at[at, 0], 1)

            @pl.when(place < sizes[axis] - 1)
            def _():
                signal(ends_sem.at[at, 0], axis, 1)

        @pl.when(place < sizes[axis] - 1)
        def _():
            pl.semaphore_wait(ends_sem.at[at, 1], 1)

            @pl.when(place > 0)
            def _():
                signal(ends_sem.at[at, 1], axis, -1)

    def down(t, y, sem):
        return send(face.at[t, 0, y], lev.at[t % 2, y, 1], lev_send.at[t], sem, "lev", -1)

    def up(t, y, sem):
        return send(face.at[t, 1, y], lev.at[t % 2, y, 0], lev_send.at[t], sem, "lev", 1)

    def send_level(t, y):
        up(t, y, lev_recv.at[t % 2, y]).start()
        down(t, y, lev_recv.at[t % 2, y]).start()

    def lon_copies(t, y):
        row = field.at[t % 2, y]
        s = t % 2
        return [
            send(row.at[0], lon.at[s, y, 1], lon_send.at[s], lon_recv.at[s, y], "lon", -1),
            send(row.at[X - 1], lon.at[s, y, 0], lon_send.at[s], lon_recv.at[s, y], "lon", 1),
        ]

    def start_lon(y, wrap):
        low, high = lon_copies(0, y)
        end = sizes["lon"] - 1

        @pl.when((places["lon"] == 0) if wrap else (places["lon"] > 0))
        def _():
            low.start()

        @pl.when((places["lon"] == end) if wrap else (places["lon"] < end))
        def _():
            high.start()

    def send_plane(t, y):
        for copy in lon_copies(t, y):
            copy.start()
        send_lat(t, y)

    def send_lat(t, y):
        s = t % 2
        if y == 0:
            send(field.at[s, 0, pl.ds(0, X)], lat.at[s, 1], lat_send.at[s], lat_recv.at[s], "lat", -1).start()
        if y == Y - 1:
            send(field.at[s, Y - 1, pl.ds(0, X)], lat.at[s, 0], lat_send.at[s], lat_recv.at[s], "lat", 1).start()

    def plane_sent(t):
        arrived(lon.at[t % 2], lon_send.at[t % 2])
        arrived(lat.at[t % 2], lat_send.at[t % 2])

    def rows_beside(t, y):
        before = field.at[t % 2, y - 1] if y > 0 else lat.at[t % 2, 0]
        after = field.at[t % 2, y + 1] if y < Y - 1 else lat.at[t % 2, 1]
        return before, after

    def start_level(y, wrap):
        @pl.when((level == levels - 1) if wrap else (level < levels - 1))
        def _():
            up(0, y, lev_recv.at[0, y]).start()

        @pl.when((level == 0) if wrap else (level > 0))
        def _():
            down(0, y, lev_recv.at[0, y]).start()

    def face_wait(group):
        for copy in faces_in[group]:
            copy.wait()

    ahead = Y // 2
    for at in range(2):
        face_wait(at)
        start_level(order[at], False)

    @pl.when((level > 0) & (level < levels - 1))
    def _():
        meet_ends("lev")
        face_wait(2)
        for y in order[2:]:
            start_level(y, False)

    @pl.when((level == 0) | (level == levels - 1))
    def _():
        face_wait(2)
        for y in order[2:ahead]:
            start_level(y, False)
        meet_ends("lev")
        for y in order[:ahead]:
            start_level(y, True)
        for y in order[ahead:]:
            start_level(y, False)
            start_level(y, True)

    for copy in f_in:
        copy.wait()
    for y in (0, Y - 1):
        send_lat(0, y)
    for y in order:
        start_lon(y, False)
    meet_ends("lon")
    for y in order:
        start_lon(y, True)

    @pl.when(level == 0)
    def _():
        below[...] = jnp.zeros_like(below)

    c_in.wait()
    place = lax.broadcasted_iota(jnp.int32, (Z, L), 0)

    def step_row(t, y):
        now, later = t % 2, (t + 1) % 2
        if y == 0:
            arrived(lat.at[now], lat_recv.at[now])
        arrived(lon.at[now, y], lon_recv.at[now, y])
        arrived(lev.at[now, y], lev_recv.at[now, y])
        before, after = rows_beside(t, y)
        field[now, y, X] = lon[now, y, 1]

        def block(at, carry):
            left, middle = carry
            start = pl.multiple_of(at * BLOCK, BLOCK)
            for i in range(BLOCK):
                x = start + i
                right = field[now, y, x + 1]
                lower = jnp.where(place == 0, lev[now, y, 0, pl.ds(x, 1), :], pltpu.roll(middle, 1, 0))
                upper = jnp.where(place == Z - 1, lev[now, y, 1, pl.ds(x, 1), :], pltpu.roll(middle, Z - 1, 0))
                around = (left + right) + (before[x] + after[x]) + (lower + upper)
                new = 0.1 * around + middle * (0.6 - 0.2 * (middle * crowd[y, x]))
                field[later, y, x] = new
                face[t + 1, 0, y, pl.ds(x, 1), :] = new[0:1]
                face[t + 1, 1, y, pl.ds(x, 1), :] = new[Z - 1 : Z]
                left, middle = middle, right
            return left, middle

        lax.fori_loop(0, X // BLOCK, block, (lon[now, y, 0], field[now, y, 0]))

    def last_row(y):
        now = LAST % 2
        if y == 0:
            arrived(lat.at[now], lat_recv.at[now])
        arrived(lon.at[now, y], lon_recv.at[now, y])
        before, after = rows_beside(LAST, y)
        field[now, y, X] = lon[now, y, 1]

        def block(at, carry):
            left, middle = carry
            start = pl.multiple_of(at * BLOCK, BLOCK)
            for i in range(BLOCK):
                x = start + i
                right = field[now, y, x + 1]
                lower = jnp.where(place == 0, 0.0, pltpu.roll(middle, 1, 0))
                upper = jnp.where(place == Z - 1, 0.0, pltpu.roll(middle, Z - 1, 0))
                around = (left + right) + (before[x] + after[x]) + (lower + upper)
                new = 0.1 * around + middle * (0.6 - 0.2 * (middle * crowd[y, x]))
                end[y, x] = new
                shift = 1
                while shift < Z:
                    new = new + jnp.where(place >= shift, pltpu.roll(new, shift, 0), 0.0)
                    shift *= 2
                scan[y, x] = new
                sums[y, pl.ds(x, 1), :] = new[Z - 1 : Z]
                left, middle = middle, right
            return left, middle

        lax.fori_loop(0, X // BLOCK, block, (lon[now, y, 0], field[now, y, 0]))

    def sum_copy(y):
        return send(sums.at[y], below.at[y], sum_send, sum_recv.at[y], "lev", 1)

    def send_sum(y, wait):
        if wait:
            sum_copy(y).wait_recv()
        from_below = below[y] + upper_part * face[LAST, 0, y]
        sums[y] = (from_below + 0.1 * face[LAST, 1, y]) + sums[y]
        sum_copy(y).start()

    def last_down(y):
        return down(LAST, y, lev_recv.at[LAST % 2, y])

    def last_up(y):
        return up(LAST, y, lev_recv.at[LAST % 2, y])

    def send_top(y):
        send(face.at[LAST, 1, y], top.at[y], lev_send.at[LAST], top_recv.at[y], "lev", -1).start()

    def relay_top(y):
        copy = send(top.at[y], top.at[y], top_send, top_recv.at[y], "lev", -1)
        copy.wait_recv()
        copy.start()

    for t in range(LAST):
        if t >= 1:
            plane_sent(t - 1)
        for at, y in enumerate(order):
            step_row(t, y)
            if t < LAST - 1:
                send_level(t + 1, y)
            send_plane(t + 1, y)
            if t < LAST - 1:
                continue

            @pl.when(level == levels - 1)
            def _():
                send_top(y)

            @pl.when(level > 0)
            def _():
                last_down(y).start()

            for k in range(1, levels - 1):
                if at < faces_first(k, Y):
                    @pl.when(level == k)
                    def _():
                        last_up(y).start()

            if at < 2:
                @pl.when(level == 0)
                def _():
                    last_down(y).start()

            done = set(order[: at + 1])
            earlier = set(order[:at])
            ready = [
                row for row in order
                if {max(row - 1, 0), row, min(row + 1, Y - 1)} <= done
                and not {max(row - 1, 0), row, min(row + 1, Y - 1)} <= earlier
            ]
            for row in ready:
                last_row(row)
                place_of = order.index(row)

                @pl.when(level == 0)
                def _():
                    send_sum(row, False)
                    if 2 <= place_of < Y - 2:
                        last_down(row).start()

    @pl.when(level == 0)
    def _():
        for y in order[max(Y - 2, 2) :]:
            last_down(y).start()
        for y in order:
            last_up(y).start()

    for k in range(1, levels - 1):
        @pl.when(level == k)
        def _():
            for kind, which in last_plan(k, levels, Y):
                y = order[which]
                if kind == "sum":
                    send_sum(y, True)
                elif kind == "face":
                    last_up(y).start()
                else:
                    relay_top(y)

    now = LAST % 2
    for y in order:
        @pl.when(level == levels - 1)
        def _():
            sum_copy(y).wait_recv()
            top[y] = face[LAST, 1, y]

        @pl.when(level == 0)
        def _():
            arrived(top.at[y], top_recv.at[y])
            lev[now, y, 0] = top[y]
            last_down(y).wait_recv()

        @pl.when(level > 0)
        def _():
            arrived(lev.at[now, y], lev_recv.at[now, y])

        base[y] = (below[y] + upper_part * face[LAST, 0, y]) + 0.1 * top[y]

        for start in range(0, X, PIECE):
            some = pl.ds(start, PIECE)
            upper = 0.1 * lev[now, y, 1, some, :]
            end[y, some, 0, :] = end[y, some, 0, :] + 0.1 * lev[now, y, 0, some, :]
            end[y, some, Z - 1, :] = end[y, some, Z - 1, :] + upper
            scan[y, some, Z - 1, :] = scan[y, some, Z - 1, :] + upper

    @pl.when(level < levels - 1)
    def _():
        arrived(sums, sum_send)

    @pl.when((level > 0) & (level < levels - 1))
    def _():
        arrived(top, top_send)

    for t in range(STEPS):
        arrived(face.at[t], lev_send.at[t])
    for t in (LAST - 1, LAST):
        plane_sent(t)


def finish(scale, end, scan, base, pot_hbm, end_hbm, pot, out_sem):
    Y, X, Z, L = pot.shape
    ends = pltpu.make_async_copy(end, end_hbm, out_sem.at[0])
    ends.start()
    for y in range(Y):
        @pl.loop(0, X // BLOCK)
        def _(at):
            start = pl.multiple_of(at * BLOCK, BLOCK)
            for i in range(BLOCK):
                x = start + i
                pot[y, x] = (scan[y, x] + base[y, pl.ds(x, 1), :]) * scale

        pltpu.make_async_copy(pot.at[y], pot_hbm.at[y], out_sem.at[1]).start()
    ends.wait()
    pltpu.make_async_copy(pot, pot_hbm, out_sem.at[1]).wait()


def per_device(sizes, field_values, crowding):
    Y, X, Z, L = field_values.shape
    f32 = jnp.float32
    dma = pltpu.SemaphoreType.DMA
    in_hbm = pl.BlockSpec(memory_space=pltpu.HBM)
    in_vmem = pl.BlockSpec(memory_space=pltpu.VMEM)
    shape = jax.ShapeDtypeStruct(field_values.shape, f32)
    end, scan, base = pl.pallas_call(
        functools.partial(march, sizes),
        out_shape=(pltpu.VMEM((Y, X, Z, L), f32), pltpu.VMEM((Y, X, Z, L), f32), pltpu.VMEM((Y, X, L), f32)),
        in_specs=[in_hbm, in_hbm],
        out_specs=(in_vmem, in_vmem, in_vmem),
        scratch_shapes=[
            pltpu.VMEM((2, Y, X + 1, Z, L), f32),
            pltpu.VMEM((Y, X, Z, L), f32),
            pltpu.VMEM((2, 2, X, Z, L), f32),
            pltpu.VMEM((2, Y, 2, Z, L), f32),
            pltpu.VMEM((2, Y, 2, X, L), f32),
            pltpu.VMEM((STEPS, 2, Y, X, L), f32),
            pltpu.VMEM((Y, X, L), f32),
            pltpu.VMEM((Y, X, L), f32),
            pltpu.VMEM((Y, X, L), f32),
            dma((4,)),
            dma((3, 2)),
            dma((2,)),
            dma((2,)),
            dma((2,)),
            dma((2, Y)),
            dma((STEPS,)),
            dma((2, Y)),
            dma,
            dma((Y,)),
            dma,
            dma((Y,)),
            pltpu.SemaphoreType.REGULAR((2, 2)),
        ],
        compiler_params=pltpu.CompilerParams(
            collective_id=0, has_side_effects=True, vmem_limit_bytes=40 * 1024 * 1024
        ),
    )(field_values, crowding)
    return pl.pallas_call(
        functools.partial(finish, 1.0 / (Z * sizes["lev"])),
        out_shape=(shape, shape),
        in_specs=[in_vmem, in_vmem, in_vmem],
        out_specs=(in_hbm, in_hbm),
        scratch_shapes=[pltpu.VMEM((Y, X, Z, L), f32), dma((2,))],
        compiler_params=pltpu.CompilerParams(vmem_limit_bytes=12 * 1024 * 1024),
    )(end, scan, base)


def solution(mesh):
    return jax.shard_map(
        functools.partial(per_device, dict(mesh.shape)),
        mesh=mesh,
        in_specs=(P("lat", "lon", "lev", None), P("lat", "lon", "lev", None)),
        out_specs=(P("lat", "lon", "lev", None), P("lat", "lon", "lev", None)),
        check_vma=False,
    )
```

```python
import functools

import jax
import jax.numpy as jnp
from jax import lax
from jax.experimental import pallas as pl
from jax.experimental.pallas import tpu as pltpu
from jax.sharding import PartitionSpec as P

STEPS = 4
BLOCK = 8
PIECE = 64


def row_order(rows):
    order = []
    for k in range((rows + 1) // 2):
        order.append(k)
        if rows - 1 - k != k:
            order.append(rows - 1 - k)
    return order


def holds(level):
    return 0 if level == 0 else 1


def last_plan(level, levels, rows):
    all_rows = list(range(rows))
    steps = [[] for _ in all_rows]

    def these(kind, places):
        return [(kind, at) for at in places]

    if level == levels - 1:
        for at in all_rows:
            steps[at].append(("top", at))
        return steps, these("low", all_rows)
    if level == 0:
        steps[0].append(("low", 0))
        end = []
        for at in all_rows[1:]:
            end += [("low", at), ("up", at - 1)]
        return steps, end + [("up", rows - 1)]
    near_top = level == levels - 2
    early_ups = rows // 2 if level == 1 and not near_top else 3 * rows // 4
    early_lows = rows // 2 if near_top else rows
    for at in all_rows:
        steps[at] += these("up", [at] if at < early_ups else []) + these("low", [at] if at < early_lows else [])
    end, top = [], 0
    for at in all_rows:
        while near_top and top < min(at + 2, rows):
            end.append(("top", top))
            top += 1
        end.append(("sum", at))
    return steps, end + these("top", all_rows[top:]) + these("up", all_rows[early_ups:]) + these("low", all_rows[early_lows:])


def march(
    sizes, f_hbm, c_hbm, end, scan, base,
    field, crowd, lat, lon, lev, face, below, sums, top,
    in_sem, face_sem, lat_send, lat_recv, lon_send, lon_recv, lev_send, lev_recv,
    top_send, top_recv, sum_send, sum_recv, ends_sem,
):
    Y, X, Z, L = crowd.shape
    order = row_order(Y)
    level = lax.axis_index("lev")
    levels = sizes["lev"]
    LAST = STEPS - 1
    gives_way = lax.axis_index("lat") == sizes["lat"] - 1
    upper_part = jnp.where(level > 0, 0.1, 0.0).astype(jnp.float32)

    def beside(axis, shift):
        n = sizes[axis]
        return {axis: lax.rem(lax.axis_index(axis) + (shift + n), n)}

    def send(src, dst, send_sem, recv_sem, axis, shift):
        return pltpu.make_async_remote_copy(
            src_ref=src, dst_ref=dst, send_sem=send_sem, recv_sem=recv_sem,
            device_id=beside(axis, shift), device_id_type=pl.DeviceIdType.MESH,
        )

    def arrived(ref, sem):
        pltpu.make_async_copy(ref, ref, sem).wait()

    groups = [pl.ds(0, 1), pl.ds(Y - 1, 1), pl.ds(1, Y - 2)]
    f_in = pltpu.make_async_copy(f_hbm, field.at[0, :, pl.ds(0, X)], in_sem.at[0])
    c_in = pltpu.make_async_copy(c_hbm, crowd, in_sem.at[1])
    for group, rows in enumerate(groups):
        pltpu.make_async_copy(f_hbm.at[rows, :, 0], face.at[0, 0, rows], face_sem.at[group]).start()
        pltpu.make_async_copy(f_hbm.at[rows, :, Z - 1], face.at[0, 1, rows], face_sem.at[group]).start()
    f_in.start()
    c_in.start()

    places = {axis: lax.axis_index(axis) for axis in ("lev", "lon")}
    barrier = pltpu.get_barrier_semaphore()

    def signal(sem, axis, shift):
        pl.semaphore_signal(sem, inc=1, device_id=beside(axis, shift), device_id_type=pl.DeviceIdType.MESH)

    greeted = 1
    for axis, place in places.items():
        @pl.when(place > 0)
        def _():
            signal(barrier, axis, -1)

        @pl.when(place < sizes[axis] - 1)
        def _():
            signal(barrier, axis, 1)

        greeted += jnp.where(place > 0, 1, 0) + jnp.where(place < sizes[axis] - 1, 1, 0)
    signal(barrier, "lat", 1)
    pl.semaphore_wait(barrier, greeted)

    for at, (axis, place) in enumerate(places.items()):
        @pl.when(place == 0)
        def _():
            signal(ends_sem.at[at, 0], axis, 1)

        @pl.when(place == sizes[axis] - 1)
        def _():
            signal(ends_sem.at[at, 1], axis, -1)

    def meet_ends(axis):
        at, place = list(places).index(axis), places[axis]

        @pl.when(place > 0)
        def _():
            pl.semaphore_wait(ends_sem.at[at, 0], 1)

            @pl.when(place < sizes[axis] - 1)
            def _():
                signal(ends_sem.at[at, 0], axis, 1)

        @pl.when(place < sizes[axis] - 1)
        def _():
            pl.semaphore_wait(ends_sem.at[at, 1], 1)

            @pl.when(place > 0)
            def _():
                signal(ends_sem.at[at, 1], axis, -1)

    def down(t, y, sem):
        return send(face.at[t, 0, y], lev.at[t % 2, y, 1], lev_send, sem, "lev", -1)

    def up(t, y, sem):
        return send(face.at[t, 1, y], lev.at[t % 2, y, 0], lev_send, sem, "lev", 1)

    def send_level(t, y):
        up(t, y, lev_recv.at[t % 2, y]).start()
        down(t, y, lev_recv.at[t % 2, y]).start()

    def lon_copies(t, y):
        row = field.at[t % 2, y]
        s = t % 2
        return [
            send(row.at[0], lon.at[s, y, 1], lon_send.at[s], lon_recv.at[s, y], "lon", -1),
            send(row.at[X - 1], lon.at[s, y, 0], lon_send.at[s], lon_recv.at[s, y], "lon", 1),
        ]

    def start_lon(y, wrap):
        low, high = lon_copies(0, y)
        end = sizes["lon"] - 1

        @pl.when((places["lon"] == 0) if wrap else (places["lon"] > 0))
        def _():
            low.start()

        @pl.when((places["lon"] == end) if wrap else (places["lon"] < end))
        def _():
            high.start()

    def send_plane(t, y):
        for copy in lon_copies(t, y):
            copy.start()
        send_lat(t, y)

    def send_lat(t, y):
        s = t % 2
        if y == 0:
            send(field.at[s, 0, pl.ds(0, X)], lat.at[s, 1], lat_send.at[s], lat_recv.at[s], "lat", -1).start()
        if y == Y - 1:
            send(field.at[s, Y - 1, pl.ds(0, X)], lat.at[s, 0], lat_send.at[s], lat_recv.at[s], "lat", 1).start()

    def plane_sent(t):
        arrived(lon.at[t % 2], lon_send.at[t % 2])
        arrived(lat.at[t % 2], lat_send.at[t % 2])

    def rows_beside(t, y):
        before = field.at[t % 2, y - 1] if y > 0 else lat.at[t % 2, 0]
        after = field.at[t % 2, y + 1] if y < Y - 1 else lat.at[t % 2, 1]
        return before, after

    def start_level(y, wrap):
        @pl.when((level == levels - 1) if wrap else (level < levels - 1))
        def _():
            up(0, y, lev_recv.at[0, y]).start()

        @pl.when((level == 0) if wrap else (level > 0))
        def _():
            down(0, y, lev_recv.at[0, y]).start()

    def face_wait(group):
        arrived(face.at[0, :, groups[group]], face_sem.at[group])

    ahead = Y // 2
    for at in range(2):
        face_wait(at)
        start_level(order[at], False)

    @pl.when((level > 0) & (level < levels - 1))
    def _():
        meet_ends("lev")
        face_wait(2)
        for y in order[2:]:
            start_level(y, False)

    @pl.when((level == 0) | (level == levels - 1))
    def _():
        face_wait(2)
        for y in order[2:ahead]:
            start_level(y, False)
        meet_ends("lev")
        for y in order[:ahead]:
            start_level(y, True)
        for y in order[ahead:]:
            start_level(y, False)
            start_level(y, True)

    f_in.wait()
    for y in (0, Y - 1):
        send_lat(0, y)
    for y in order:
        start_lon(y, False)
    meet_ends("lon")
    for y in order:
        start_lon(y, True)

    @pl.when(level == 0)
    def _():
        below[...] = jnp.zeros_like(below)

    c_in.wait()
    place = lax.broadcasted_iota(jnp.int32, (Z, L), 0)

    def step_row(t, y):
        now, later = t % 2, (t + 1) % 2
        if y == 0:
            arrived(lat.at[now], lat_recv.at[now])
        arrived(lon.at[now, y], lon_recv.at[now, y])
        arrived(lev.at[now, y], lev_recv.at[now, y])
        before, after = rows_beside(t, y)
        field[now, y, X] = lon[now, y, 1]

        def block(at, carry):
            left, middle = carry
            start = pl.multiple_of(at * BLOCK, BLOCK)
            for i in range(BLOCK):
                x = start + i
                right = field[now, y, x + 1]
                lower = jnp.where(place == 0, lev[now, y, 0, pl.ds(x, 1), :], pltpu.roll(middle, 1, 0))
                upper = jnp.where(place == Z - 1, lev[now, y, 1, pl.ds(x, 1), :], pltpu.roll(middle, Z - 1, 0))
                around = (left + right) + (before[x] + after[x]) + (lower + upper)
                new = 0.1 * around + middle * (0.6 - 0.2 * (middle * crowd[y, x]))
                field[later, y, x] = new
                face[t + 1, 0, y, pl.ds(x, 1), :] = new[0:1]
                face[t + 1, 1, y, pl.ds(x, 1), :] = new[Z - 1 : Z]
                left, middle = middle, right
            return left, middle

        lax.fori_loop(0, X // BLOCK, block, (lon[now, y, 0], field[now, y, 0]))

    def last_row(y):
        now = LAST % 2
        if y == 0:
            arrived(lat.at[now], lat_recv.at[now])
        arrived(lon.at[now, y], lon_recv.at[now, y])
        before, after = rows_beside(LAST, y)
        field[now, y, X] = lon[now, y, 1]

        def block(at, carry):
            left, middle = carry
            start = pl.multiple_of(at * BLOCK, BLOCK)
            for i in range(BLOCK):
                x = start + i
                right = field[now, y, x + 1]
                lower = jnp.where(place == 0, 0.0, pltpu.roll(middle, 1, 0))
                upper = jnp.where(place == Z - 1, 0.0, pltpu.roll(middle, Z - 1, 0))
                around = (left + right) + (before[x] + after[x]) + (lower + upper)
                new = 0.1 * around + middle * (0.6 - 0.2 * (middle * crowd[y, x]))
                end[y, x] = new
                shift = 1
                while shift < Z:
                    new = new + jnp.where(place >= shift, pltpu.roll(new, shift, 0), 0.0)
                    shift *= 2
                scan[y, x] = new
                sums[y, pl.ds(x, 1), :] = new[Z - 1 : Z]
                left, middle = middle, right
            return left, middle

        lax.fori_loop(0, X // BLOCK, block, (lon[now, y, 0], field[now, y, 0]))

    def sum_copy(y):
        return send(sums.at[y], below.at[y], sum_send, sum_recv.at[y], "lev", 1)

    def send_sum(y, wait):
        if wait:
            sum_copy(y).wait_recv()
        from_below = below[y] + upper_part * face[LAST, 0, y]
        sums[y] = (from_below + 0.1 * face[LAST, 1, y]) + sums[y]
        sum_copy(y).start()

    def last_down(y):
        return down(LAST, y, lev_recv.at[LAST % 2, y])

    def last_up(y):
        return up(LAST, y, lev_recv.at[LAST % 2, y])

    def send_top(y):
        send(face.at[LAST, 1, y], top.at[y], lev_send, top_recv.at[y], "lev", -1).start()

    def relay_top(y):
        copy = send(top.at[y], top.at[y], top_send, top_recv.at[y], "lev", -1)
        copy.wait_recv()
        copy.start()

    plans = [last_plan(k, levels, Y) for k in range(levels)]

    def act(k, kind, which):
        y = order[which]
        if kind == "sum":
            send_sum(y, True)
        elif kind == "up" and which >= Y - holds(k):
            @pl.when(~gives_way)
            def _():
                last_up(y).start()
        elif kind == "up":
            last_up(y).start()
        elif kind == "low":
            last_down(y).start()
        elif k == levels - 1:
            send_top(y)
        else:
            relay_top(y)

    for t in range(LAST):
        if t >= 1:
            plane_sent(t - 1)
        for at, y in enumerate(order):
            step_row(t, y)
            if t < LAST - 1:
                send_level(t + 1, y)
            send_plane(t + 1, y)
            if t < LAST - 1:
                continue

            for k in range(levels):
                if plans[k][0][at]:
                    @pl.when(level == k)
                    def _():
                        for kind, which in plans[k][0][at]:
                            act(k, kind, which)

            done = set(order[: at + 1])
            earlier = set(order[:at])
            ready = [
                row for row in order
                if {max(row - 1, 0), row, min(row + 1, Y - 1)} <= done
                and not {max(row - 1, 0), row, min(row + 1, Y - 1)} <= earlier
            ]
            for row in ready:
                last_row(row)

                @pl.when(level == 0)
                def _():
                    send_sum(row, False)

    for k in range(levels):
        @pl.when(level == k)
        def _():
            for kind, which in plans[k][1]:
                act(k, kind, which)

    now = LAST % 2
    for at, y in enumerate(order):
        @pl.when(level == levels - 1)
        def _():
            sum_copy(y).wait_recv()
            top[y] = face[LAST, 1, y]

        @pl.when(level == 0)
        def _():
            arrived(top.at[y], top_recv.at[y])
            lev[now, y, 0] = top[y]

        base[y] = (below[y] + upper_part * face[LAST, 0, y]) + 0.1 * top[y]

        @pl.when(level == 0)
        def _():
            last_down(y).wait_recv()

        @pl.when(level > 0)
        def _():
            arrived(lev.at[now, y], lev_recv.at[now, y])

        if at == max(Y - 3, 0):
            for k in range(levels - 1):
                @pl.when((level == k) & gives_way)
                def _():
                    for held in order[Y - holds(k) :]:
                        last_up(held).start()

        for start in range(0, X, PIECE):
            some = pl.ds(start, PIECE)
            upper = 0.1 * lev[now, y, 1, some, :]
            end[y, some, 0, :] = end[y, some, 0, :] + 0.1 * lev[now, y, 0, some, :]
            end[y, some, Z - 1, :] = end[y, some, Z - 1, :] + upper
            scan[y, some, Z - 1, :] = scan[y, some, Z - 1, :] + upper

    @pl.when(level < levels - 1)
    def _():
        arrived(sums, sum_send)

    @pl.when((level > 0) & (level < levels - 1))
    def _():
        arrived(top, top_send)

    arrived(face, lev_send)
    for t in (LAST - 1, LAST):
        plane_sent(t)


def finish(scale, end, scan, base, pot_hbm, end_hbm, pot, out_sem):
    Y, X, Z, L = pot.shape
    ends = pltpu.make_async_copy(end, end_hbm, out_sem.at[0])
    ends.start()
    for y in range(Y):
        @pl.loop(0, X // BLOCK)
        def _(at):
            start = pl.multiple_of(at * BLOCK, BLOCK)
            for i in range(BLOCK):
                x = start + i
                pot[y, x] = (scan[y, x] + base[y, pl.ds(x, 1), :]) * scale

        pltpu.make_async_copy(pot.at[y], pot_hbm.at[y], out_sem.at[1]).start()
    ends.wait()
    pltpu.make_async_copy(pot, pot_hbm, out_sem.at[1]).wait()


def per_device(sizes, field_values, crowding):
    Y, X, Z, L = field_values.shape
    f32 = jnp.float32
    dma = pltpu.SemaphoreType.DMA
    in_hbm = pl.BlockSpec(memory_space=pltpu.HBM)
    in_vmem = pl.BlockSpec(memory_space=pltpu.VMEM)
    shape = jax.ShapeDtypeStruct(field_values.shape, f32)
    end, scan, base = pl.pallas_call(
        functools.partial(march, sizes),
        out_shape=(pltpu.VMEM((Y, X, Z, L), f32), pltpu.VMEM((Y, X, Z, L), f32), pltpu.VMEM((Y, X, L), f32)),
        in_specs=[in_hbm, in_hbm],
        out_specs=(in_vmem, in_vmem, in_vmem),
        scratch_shapes=[
            pltpu.VMEM((2, Y, X + 1, Z, L), f32),
            pltpu.VMEM((Y, X, Z, L), f32),
            pltpu.VMEM((2, 2, X, Z, L), f32),
            pltpu.VMEM((2, Y, 2, Z, L), f32),
            pltpu.VMEM((2, Y, 2, X, L), f32),
            pltpu.VMEM((STEPS, 2, Y, X, L), f32),
            pltpu.VMEM((Y, X, L), f32),
            pltpu.VMEM((Y, X, L), f32),
            pltpu.VMEM((Y, X, L), f32),
            dma((2,)),
            dma((3,)),
            dma((2,)),
            dma((2,)),
            dma((2,)),
            dma((2, Y)),
            dma,
            dma((2, Y)),
            dma,
            dma((Y,)),
            dma,
            dma((Y,)),
            pltpu.SemaphoreType.REGULAR((2, 2)),
        ],
        compiler_params=pltpu.CompilerParams(
            collective_id=0, has_side_effects=True, vmem_limit_bytes=40 * 1024 * 1024
        ),
    )(field_values, crowding)
    return pl.pallas_call(
        functools.partial(finish, 1.0 / (Z * sizes["lev"])),
        out_shape=(shape, shape),
        in_specs=[in_vmem, in_vmem, in_vmem],
        out_specs=(in_hbm, in_hbm),
        scratch_shapes=[pltpu.VMEM((Y, X, Z, L), f32), dma((2,))],
        compiler_params=pltpu.CompilerParams(vmem_limit_bytes=12 * 1024 * 1024),
    )(end, scan, base)


def solution(mesh):
    return jax.shard_map(
        functools.partial(per_device, dict(mesh.shape)),
        mesh=mesh,
        in_specs=(P("lat", "lon", "lev", None), P("lat", "lon", "lev", None)),
        out_specs=(P("lat", "lon", "lev", None), P("lat", "lon", "lev", None)),
        check_vma=False,
    )
```

```python
import functools

import jax
import jax.numpy as jnp
from jax import lax
from jax.experimental import pallas as pl
from jax.experimental.pallas import tpu as pltpu
from jax.sharding import PartitionSpec as P

STEPS = 4
BLOCK = 8
PIECE = 64


def row_order(rows):
    order = []
    for k in range((rows + 1) // 2):
        order.append(k)
        if rows - 1 - k != k:
            order.append(rows - 1 - k)
    return order


def holds(level):
    return 0 if level == 0 else 1


def last_plan(level, levels, rows):
    all_rows = list(range(rows))
    steps = [[] for _ in all_rows]

    def these(kind, places):
        return [(kind, at) for at in places]

    if level == levels - 1:
        for at in all_rows:
            steps[at].append(("top", at))
        return steps, these("low", all_rows)
    if level == 0:
        steps[0].append(("low", 0))
        end = []
        for at in all_rows[1:]:
            end += [("up", at - 1), ("low", at)]
        return steps, end + [("up", rows - 1)]
    near_top = level == levels - 2
    early_ups = rows // 2 if level == 1 and not near_top else 3 * rows // 4
    early_lows = rows // 2 if near_top else rows
    for at in all_rows:
        steps[at] += these("up", [at] if at < early_ups else []) + these("low", [at] if at < early_lows else [])
    end, top = [], 0
    for at in all_rows:
        while near_top and top < min(at + 2, rows):
            end.append(("top", top))
            top += 1
        end.append(("sum", at))
    return steps, end + these("top", all_rows[top:]) + these("up", all_rows[early_ups:]) + these("low", all_rows[early_lows:])


def march(
    sizes, f_hbm, c_hbm, end, scan, base,
    field, crowd, lat, lon, lev, face, below, sums, top,
    in_sem, face_sem, lat_send, lat_recv, lon_send, lon_recv, lev_send, lev_recv,
    top_send, top_recv, sum_send, sum_recv, ends_sem,
):
    Y, X, Z, L = crowd.shape
    order = row_order(Y)
    level = lax.axis_index("lev")
    levels = sizes["lev"]
    LAST = STEPS - 1
    gives_way = lax.axis_index("lat") == sizes["lat"] - 1
    upper_part = jnp.where(level > 0, 0.1, 0.0).astype(jnp.float32)

    def beside(axis, shift):
        n = sizes[axis]
        return {axis: lax.rem(lax.axis_index(axis) + (shift + n), n)}

    def send(src, dst, send_sem, recv_sem, axis, shift):
        return pltpu.make_async_remote_copy(
            src_ref=src, dst_ref=dst, send_sem=send_sem, recv_sem=recv_sem,
            device_id=beside(axis, shift), device_id_type=pl.DeviceIdType.MESH,
        )

    def arrived(ref, sem):
        pltpu.make_async_copy(ref, ref, sem).wait()

    groups = [pl.ds(0, 1), pl.ds(Y - 1, 1), pl.ds(1, Y - 2)]
    f_in = pltpu.make_async_copy(f_hbm, field.at[0, :, pl.ds(0, X)], in_sem.at[0])
    c_in = pltpu.make_async_copy(c_hbm, crowd, in_sem.at[1])
    for group, rows in enumerate(groups):
        pltpu.make_async_copy(f_hbm.at[rows, :, 0], face.at[0, 0, rows], face_sem.at[group]).start()
        pltpu.make_async_copy(f_hbm.at[rows, :, Z - 1], face.at[0, 1, rows], face_sem.at[group]).start()
    f_in.start()
    c_in.start()

    places = {axis: lax.axis_index(axis) for axis in ("lev", "lon")}
    barrier = pltpu.get_barrier_semaphore()

    def signal(sem, axis, shift):
        pl.semaphore_signal(sem, inc=1, device_id=beside(axis, shift), device_id_type=pl.DeviceIdType.MESH)

    greeted = 1
    for axis, place in places.items():
        @pl.when(place > 0)
        def _():
            signal(barrier, axis, -1)

        @pl.when(place < sizes[axis] - 1)
        def _():
            signal(barrier, axis, 1)

        greeted += jnp.where(place > 0, 1, 0) + jnp.where(place < sizes[axis] - 1, 1, 0)
    signal(barrier, "lat", 1)
    pl.semaphore_wait(barrier, greeted)

    for at, (axis, place) in enumerate(places.items()):
        @pl.when(place == 0)
        def _():
            signal(ends_sem.at[at, 0], axis, 1)

        @pl.when(place == sizes[axis] - 1)
        def _():
            signal(ends_sem.at[at, 1], axis, -1)

    def meet_ends(axis):
        at, place = list(places).index(axis), places[axis]

        @pl.when(place > 0)
        def _():
            pl.semaphore_wait(ends_sem.at[at, 0], 1)

            @pl.when(place < sizes[axis] - 1)
            def _():
                signal(ends_sem.at[at, 0], axis, 1)

        @pl.when(place < sizes[axis] - 1)
        def _():
            pl.semaphore_wait(ends_sem.at[at, 1], 1)

            @pl.when(place > 0)
            def _():
                signal(ends_sem.at[at, 1], axis, -1)

    def down(t, y, sem):
        return send(face.at[t, 0, y], lev.at[t % 2, y, 1], lev_send, sem, "lev", -1)

    def up(t, y, sem):
        return send(face.at[t, 1, y], lev.at[t % 2, y, 0], lev_send, sem, "lev", 1)

    def send_level(t, y):
        up(t, y, lev_recv.at[t % 2, y]).start()
        down(t, y, lev_recv.at[t % 2, y]).start()

    def lon_copies(t, y):
        row = field.at[t % 2, y]
        s = t % 2
        return [
            send(row.at[0], lon.at[s, y, 1], lon_send.at[s], lon_recv.at[s, y], "lon", -1),
            send(row.at[X - 1], lon.at[s, y, 0], lon_send.at[s], lon_recv.at[s, y], "lon", 1),
        ]

    def start_lon(y, wrap):
        low, high = lon_copies(0, y)
        end = sizes["lon"] - 1

        @pl.when((places["lon"] == 0) if wrap else (places["lon"] > 0))
        def _():
            low.start()

        @pl.when((places["lon"] == end) if wrap else (places["lon"] < end))
        def _():
            high.start()

    def send_plane(t, y):
        for copy in lon_copies(t, y):
            copy.start()
        send_lat(t, y)

    def send_lat(t, y):
        s = t % 2
        if y == 0:
            send(field.at[s, 0, pl.ds(0, X)], lat.at[s, 1], lat_send.at[s], lat_recv.at[s], "lat", -1).start()
        if y == Y - 1:
            send(field.at[s, Y - 1, pl.ds(0, X)], lat.at[s, 0], lat_send.at[s], lat_recv.at[s], "lat", 1).start()

    def plane_sent(t):
        arrived(lon.at[t % 2], lon_send.at[t % 2])
        arrived(lat.at[t % 2], lat_send.at[t % 2])

    def rows_beside(t, y):
        before = field.at[t % 2, y - 1] if y > 0 else lat.at[t % 2, 0]
        after = field.at[t % 2, y + 1] if y < Y - 1 else lat.at[t % 2, 1]
        return before, after

    def start_level(y, wrap):
        @pl.when((level == levels - 1) if wrap else (level < levels - 1))
        def _():
            up(0, y, lev_recv.at[0, y]).start()

        @pl.when((level == 0) if wrap else (level > 0))
        def _():
            down(0, y, lev_recv.at[0, y]).start()

    def face_wait(group):
        arrived(face.at[0, :, groups[group]], face_sem.at[group])

    ahead = Y // 2
    for at in range(2):
        face_wait(at)
        start_level(order[at], False)

    @pl.when((level > 0) & (level < levels - 1))
    def _():
        meet_ends("lev")
        face_wait(2)
        for y in order[2:]:
            start_level(y, False)

    @pl.when((level == 0) | (level == levels - 1))
    def _():
        face_wait(2)
        for y in order[2:ahead]:
            start_level(y, False)
        meet_ends("lev")
        for y in order[:ahead]:
            start_level(y, True)
        for y in order[ahead:]:
            start_level(y, False)
            start_level(y, True)

    f_in.wait()
    for y in (0, Y - 1):
        send_lat(0, y)
    for y in order:
        start_lon(y, False)
    meet_ends("lon")
    for y in order:
        start_lon(y, True)

    @pl.when(level == 0)
    def _():
        below[...] = jnp.zeros_like(below)

    c_in.wait()
    place = lax.broadcasted_iota(jnp.int32, (Z, L), 0)

    def step_row(t, y):
        now, later = t % 2, (t + 1) % 2
        if y == 0:
            arrived(lat.at[now], lat_recv.at[now])
        arrived(lon.at[now, y], lon_recv.at[now, y])
        arrived(lev.at[now, y], lev_recv.at[now, y])
        before, after = rows_beside(t, y)
        field[now, y, X] = lon[now, y, 1]

        def block(at, carry):
            left, middle = carry
            start = pl.multiple_of(at * BLOCK, BLOCK)
            for i in range(BLOCK):
                x = start + i
                right = field[now, y, x + 1]
                lower = jnp.where(place == 0, lev[now, y, 0, pl.ds(x, 1), :], pltpu.roll(middle, 1, 0))
                upper = jnp.where(place == Z - 1, lev[now, y, 1, pl.ds(x, 1), :], pltpu.roll(middle, Z - 1, 0))
                around = (left + right) + (before[x] + after[x]) + (lower + upper)
                new = 0.1 * around + middle * (0.6 - 0.2 * (middle * crowd[y, x]))
                field[later, y, x] = new
                face[t + 1, 0, y, pl.ds(x, 1), :] = new[0:1]
                face[t + 1, 1, y, pl.ds(x, 1), :] = new[Z - 1 : Z]
                left, middle = middle, right
            return left, middle

        lax.fori_loop(0, X // BLOCK, block, (lon[now, y, 0], field[now, y, 0]))

    def last_row(y):
        now = LAST % 2
        if y == 0:
            arrived(lat.at[now], lat_recv.at[now])
        arrived(lon.at[now, y], lon_recv.at[now, y])
        before, after = rows_beside(LAST, y)
        field[now, y, X] = lon[now, y, 1]

        def block(at, carry):
            left, middle = carry
            start = pl.multiple_of(at * BLOCK, BLOCK)
            for i in range(BLOCK):
                x = start + i
                right = field[now, y, x + 1]
                lower = jnp.where(place == 0, 0.0, pltpu.roll(middle, 1, 0))
                upper = jnp.where(place == Z - 1, 0.0, pltpu.roll(middle, Z - 1, 0))
                around = (left + right) + (before[x] + after[x]) + (lower + upper)
                new = 0.1 * around + middle * (0.6 - 0.2 * (middle * crowd[y, x]))
                end[y, x] = new
                shift = 1
                while shift < Z:
                    new = new + jnp.where(place >= shift, pltpu.roll(new, shift, 0), 0.0)
                    shift *= 2
                scan[y, x] = new
                sums[y, pl.ds(x, 1), :] = new[Z - 1 : Z]
                left, middle = middle, right
            return left, middle

        lax.fori_loop(0, X // BLOCK, block, (lon[now, y, 0], field[now, y, 0]))

    def sum_copy(y):
        return send(sums.at[y], below.at[y], sum_send, sum_recv.at[y], "lev", 1)

    def send_sum(y, wait):
        if wait:
            sum_copy(y).wait_recv()
        from_below = below[y] + upper_part * face[LAST, 0, y]
        sums[y] = (from_below + 0.1 * face[LAST, 1, y]) + sums[y]
        sum_copy(y).start()

    def last_down(y):
        return down(LAST, y, lev_recv.at[LAST % 2, y])

    def last_up(y):
        return up(LAST, y, lev_recv.at[LAST % 2, y])

    def send_top(y):
        send(face.at[LAST, 1, y], top.at[y], lev_send, top_recv.at[y], "lev", -1).start()

    def relay_top(y):
        copy = send(top.at[y], top.at[y], top_send, top_recv.at[y], "lev", -1)
        copy.wait_recv()
        copy.start()

    plans = [last_plan(k, levels, Y) for k in range(levels)]

    def act(k, kind, which):
        y = order[which]
        if kind == "sum":
            send_sum(y, True)
        elif kind == "up" and which >= Y - holds(k):
            @pl.when(~gives_way)
            def _():
                last_up(y).start()
        elif kind == "up":
            last_up(y).start()
        elif kind == "low":
            last_down(y).start()
        elif k == levels - 1:
            send_top(y)
        else:
            relay_top(y)

    for t in range(LAST):
        if t >= 1:
            plane_sent(t - 1)
        for at, y in enumerate(order):
            step_row(t, y)
            if t < LAST - 1:
                send_level(t + 1, y)
            send_plane(t + 1, y)
            if t < LAST - 1:
                continue

            for k in range(levels):
                if plans[k][0][at]:
                    @pl.when(level == k)
                    def _():
                        for kind, which in plans[k][0][at]:
                            act(k, kind, which)

            done = set(order[: at + 1])
            earlier = set(order[:at])
            ready = [
                row for row in order
                if {max(row - 1, 0), row, min(row + 1, Y - 1)} <= done
                and not {max(row - 1, 0), row, min(row + 1, Y - 1)} <= earlier
            ]
            for row in ready:
                last_row(row)

                @pl.when(level == 0)
                def _():
                    send_sum(row, False)

    for k in range(levels):
        @pl.when(level == k)
        def _():
            for kind, which in plans[k][1]:
                act(k, kind, which)

    now = LAST % 2
    for at, y in enumerate(order):
        @pl.when(level == levels - 1)
        def _():
            sum_copy(y).wait_recv()
            top[y] = face[LAST, 1, y]

        @pl.when(level == 0)
        def _():
            arrived(top.at[y], top_recv.at[y])
            lev[now, y, 0] = top[y]

        base[y] = (below[y] + upper_part * face[LAST, 0, y]) + 0.1 * top[y]

        @pl.when(level == 0)
        def _():
            last_down(y).wait_recv()

        @pl.when(level > 0)
        def _():
            arrived(lev.at[now, y], lev_recv.at[now, y])

        if at == max(Y - 3, 0):
            for k in range(levels - 1):
                @pl.when((level == k) & gives_way)
                def _():
                    for held in order[Y - holds(k) :]:
                        last_up(held).start()

        for start in range(0, X, PIECE):
            some = pl.ds(start, PIECE)
            upper = 0.1 * lev[now, y, 1, some, :]
            end[y, some, 0, :] = end[y, some, 0, :] + 0.1 * lev[now, y, 0, some, :]
            end[y, some, Z - 1, :] = end[y, some, Z - 1, :] + upper
            scan[y, some, Z - 1, :] = scan[y, some, Z - 1, :] + upper

    @pl.when(level < levels - 1)
    def _():
        arrived(sums, sum_send)

    @pl.when((level > 0) & (level < levels - 1))
    def _():
        arrived(top, top_send)

    arrived(face, lev_send)
    for t in (LAST - 1, LAST):
        plane_sent(t)


def finish(scale, end, scan, base, pot_hbm, end_hbm, pot, out_sem):
    Y, X, Z, L = pot.shape
    part = X // 4
    for y in range(Y):
        for x in range(0, X, part):
            some = pl.ds(x, part)
            pltpu.make_async_copy(end.at[y, some], end_hbm.at[y, some], out_sem.at[0]).start()
    for y in range(Y):
        @pl.loop(0, X // BLOCK)
        def _(at):
            start = pl.multiple_of(at * BLOCK, BLOCK)
            for i in range(BLOCK):
                x = start + i
                pot[y, x] = (scan[y, x] + base[y, pl.ds(x, 1), :]) * scale

        for x in range(0, X, part):
            some = pl.ds(x, part)
            pltpu.make_async_copy(pot.at[y, some], pot_hbm.at[y, some], out_sem.at[1]).start()
    pltpu.make_async_copy(end, end_hbm, out_sem.at[0]).wait()
    pltpu.make_async_copy(pot, pot_hbm, out_sem.at[1]).wait()


def per_device(sizes, field_values, crowding):
    Y, X, Z, L = field_values.shape
    f32 = jnp.float32
    dma = pltpu.SemaphoreType.DMA
    in_hbm = pl.BlockSpec(memory_space=pltpu.HBM)
    in_vmem = pl.BlockSpec(memory_space=pltpu.VMEM)
    shape = jax.ShapeDtypeStruct(field_values.shape, f32)
    end, scan, base = pl.pallas_call(
        functools.partial(march, sizes),
        out_shape=(pltpu.VMEM((Y, X, Z, L), f32), pltpu.VMEM((Y, X, Z, L), f32), pltpu.VMEM((Y, X, L), f32)),
        in_specs=[in_hbm, in_hbm],
        out_specs=(in_vmem, in_vmem, in_vmem),
        scratch_shapes=[
            pltpu.VMEM((2, Y, X + 1, Z, L), f32),
            pltpu.VMEM((Y, X, Z, L), f32),
            pltpu.VMEM((2, 2, X, Z, L), f32),
            pltpu.VMEM((2, Y, 2, Z, L), f32),
            pltpu.VMEM((2, Y, 2, X, L), f32),
            pltpu.VMEM((STEPS, 2, Y, X, L), f32),
            pltpu.VMEM((Y, X, L), f32),
            pltpu.VMEM((Y, X, L), f32),
            pltpu.VMEM((Y, X, L), f32),
            dma((2,)),
            dma((3,)),
            dma((2,)),
            dma((2,)),
            dma((2,)),
            dma((2, Y)),
            dma,
            dma((2, Y)),
            dma,
            dma((Y,)),
            dma,
            dma((Y,)),
            pltpu.SemaphoreType.REGULAR((2, 2)),
        ],
        compiler_params=pltpu.CompilerParams(
            collective_id=0, has_side_effects=True, vmem_limit_bytes=40 * 1024 * 1024
        ),
    )(field_values, crowding)
    return pl.pallas_call(
        functools.partial(finish, 1.0 / (Z * sizes["lev"])),
        out_shape=(shape, shape),
        in_specs=[in_vmem, in_vmem, in_vmem],
        out_specs=(in_hbm, in_hbm),
        scratch_shapes=[pltpu.VMEM((Y, X, Z, L), f32), dma((2,))],
        compiler_params=pltpu.CompilerParams(vmem_limit_bytes=12 * 1024 * 1024),
    )(end, scan, base)


def solution(mesh):
    return jax.shard_map(
        functools.partial(per_device, dict(mesh.shape)),
        mesh=mesh,
        in_specs=(P("lat", "lon", "lev", None), P("lat", "lon", "lev", None)),
        out_specs=(P("lat", "lon", "lev", None), P("lat", "lon", "lev", None)),
        check_vma=False,
    )
```

```python
import functools

import jax
import jax.numpy as jnp
from jax import lax
from jax.experimental import pallas as pl
from jax.experimental.pallas import tpu as pltpu
from jax.sharding import PartitionSpec as P

STEPS = 4
BLOCK = 8
PIECE = 64


def row_order(rows):
    order = []
    for k in range((rows + 1) // 2):
        order.append(k)
        if rows - 1 - k != k:
            order.append(rows - 1 - k)
    return order


def holds(level):
    return 0 if level == 0 else 1


def last_plan(level, levels, rows):
    all_rows = list(range(rows))
    steps = [[] for _ in all_rows]

    def these(kind, places):
        return [(kind, at) for at in places]

    if level == levels - 1:
        for at in all_rows:
            steps[at].append(("top", at))
        return steps, these("low", all_rows)
    if level == 0:
        steps[0].append(("low", 0))
        end = []
        for at in all_rows[1:]:
            end += [("up", at - 1), ("low", at)]
        return steps, end + [("up", rows - 1)]
    near_top = level == levels - 2
    early_ups = rows // 2 if level == 1 and not near_top else 3 * rows // 4
    early_lows = rows // 2 if near_top else rows
    for at in all_rows:
        steps[at] += these("up", [at] if at < early_ups else []) + these("low", [at] if at < early_lows else [])
    end, top = [], 0
    for at in all_rows:
        while near_top and top < min(at + 2, rows):
            end.append(("top", top))
            top += 1
        end.append(("sum", at))
    return steps, end + these("up", all_rows[early_ups:]) + these("top", all_rows[top:]) + these("low", all_rows[early_lows:])


def march(
    sizes, f_hbm, c_hbm, end, scan, base,
    field, crowd, lat, lon, lev, face, below, sums, top,
    in_sem, face_sem, lat_send, lat_recv, lon_send, lon_recv, lev_send, lev_recv,
    top_send, top_recv, sum_send, sum_recv, ends_sem,
):
    Y, X, Z, L = crowd.shape
    order = row_order(Y)
    level = lax.axis_index("lev")
    levels = sizes["lev"]
    LAST = STEPS - 1
    gives_way = lax.axis_index("lat") == sizes["lat"] - 1
    upper_part = jnp.where(level > 0, 0.1, 0.0).astype(jnp.float32)

    def beside(axis, shift):
        n = sizes[axis]
        return {axis: lax.rem(lax.axis_index(axis) + (shift + n), n)}

    def send(src, dst, send_sem, recv_sem, axis, shift):
        return pltpu.make_async_remote_copy(
            src_ref=src, dst_ref=dst, send_sem=send_sem, recv_sem=recv_sem,
            device_id=beside(axis, shift), device_id_type=pl.DeviceIdType.MESH,
        )

    def arrived(ref, sem):
        pltpu.make_async_copy(ref, ref, sem).wait()

    groups = [pl.ds(0, 1), pl.ds(Y - 1, 1), pl.ds(1, Y - 2)]
    f_in = pltpu.make_async_copy(f_hbm, field.at[0, :, pl.ds(0, X)], in_sem.at[0])
    c_in = pltpu.make_async_copy(c_hbm, crowd, in_sem.at[1])
    for group, rows in enumerate(groups):
        pltpu.make_async_copy(f_hbm.at[rows, :, 0], face.at[0, 0, rows], face_sem.at[group]).start()
        pltpu.make_async_copy(f_hbm.at[rows, :, Z - 1], face.at[0, 1, rows], face_sem.at[group]).start()
    f_in.start()
    c_in.start()

    places = {axis: lax.axis_index(axis) for axis in ("lev", "lon")}
    barrier = pltpu.get_barrier_semaphore()

    def signal(sem, axis, shift):
        pl.semaphore_signal(sem, inc=1, device_id=beside(axis, shift), device_id_type=pl.DeviceIdType.MESH)

    greeted = 1
    for axis, place in places.items():
        @pl.when(place > 0)
        def _():
            signal(barrier, axis, -1)

        @pl.when(place < sizes[axis] - 1)
        def _():
            signal(barrier, axis, 1)

        greeted += jnp.where(place > 0, 1, 0) + jnp.where(place < sizes[axis] - 1, 1, 0)
    signal(barrier, "lat", 1)
    pl.semaphore_wait(barrier, greeted)

    for at, (axis, place) in enumerate(places.items()):
        @pl.when(place == 0)
        def _():
            signal(ends_sem.at[at, 0], axis, 1)

        @pl.when(place == sizes[axis] - 1)
        def _():
            signal(ends_sem.at[at, 1], axis, -1)

    def meet_ends(axis):
        at, place = list(places).index(axis), places[axis]

        @pl.when(place > 0)
        def _():
            pl.semaphore_wait(ends_sem.at[at, 0], 1)

            @pl.when(place < sizes[axis] - 1)
            def _():
                signal(ends_sem.at[at, 0], axis, 1)

        @pl.when(place < sizes[axis] - 1)
        def _():
            pl.semaphore_wait(ends_sem.at[at, 1], 1)

            @pl.when(place > 0)
            def _():
                signal(ends_sem.at[at, 1], axis, -1)

    def down(t, y, sem):
        return send(face.at[t, 0, y], lev.at[t % 2, y, 1], lev_send, sem, "lev", -1)

    def up(t, y, sem):
        return send(face.at[t, 1, y], lev.at[t % 2, y, 0], lev_send, sem, "lev", 1)

    def send_level(t, y):
        up(t, y, lev_recv.at[t % 2, y]).start()
        down(t, y, lev_recv.at[t % 2, y]).start()

    def lon_copies(t, y):
        row = field.at[t % 2, y]
        s = t % 2
        return [
            send(row.at[0], lon.at[s, y, 1], lon_send.at[s], lon_recv.at[s, y], "lon", -1),
            send(row.at[X - 1], lon.at[s, y, 0], lon_send.at[s], lon_recv.at[s, y], "lon", 1),
        ]

    def start_lon(y, wrap):
        low, high = lon_copies(0, y)
        end = sizes["lon"] - 1

        @pl.when((places["lon"] == 0) if wrap else (places["lon"] > 0))
        def _():
            low.start()

        @pl.when((places["lon"] == end) if wrap else (places["lon"] < end))
        def _():
            high.start()

    def send_plane(t, y):
        for copy in lon_copies(t, y):
            copy.start()
        send_lat(t, y)

    def send_lat(t, y):
        s = t % 2
        if y == 0:
            send(field.at[s, 0, pl.ds(0, X)], lat.at[s, 1], lat_send.at[s], lat_recv.at[s], "lat", -1).start()
        if y == Y - 1:
            send(field.at[s, Y - 1, pl.ds(0, X)], lat.at[s, 0], lat_send.at[s], lat_recv.at[s], "lat", 1).start()

    def plane_sent(t):
        arrived(lon.at[t % 2], lon_send.at[t % 2])
        arrived(lat.at[t % 2], lat_send.at[t % 2])

    def rows_beside(t, y):
        before = field.at[t % 2, y - 1] if y > 0 else lat.at[t % 2, 0]
        after = field.at[t % 2, y + 1] if y < Y - 1 else lat.at[t % 2, 1]
        return before, after

    def start_level(y, wrap):
        @pl.when((level == levels - 1) if wrap else (level < levels - 1))
        def _():
            up(0, y, lev_recv.at[0, y]).start()

        @pl.when((level == 0) if wrap else (level > 0))
        def _():
            down(0, y, lev_recv.at[0, y]).start()

    def face_wait(group):
        arrived(face.at[0, :, groups[group]], face_sem.at[group])

    ahead = Y // 2
    for at in range(2):
        face_wait(at)
        start_level(order[at], False)

    @pl.when((level > 0) & (level < levels - 1))
    def _():
        meet_ends("lev")
        face_wait(2)
        for y in order[2:]:
            start_level(y, False)

    @pl.when((level == 0) | (level == levels - 1))
    def _():
        face_wait(2)
        for y in order[2:ahead]:
            start_level(y, False)
        meet_ends("lev")
        for y in order[:ahead]:
            start_level(y, True)
        for y in order[ahead:]:
            start_level(y, False)
            start_level(y, True)

    f_in.wait()
    for y in (0, Y - 1):
        send_lat(0, y)
    for y in order:
        start_lon(y, False)
    meet_ends("lon")
    for y in order:
        start_lon(y, True)

    @pl.when(level == 0)
    def _():
        below[...] = jnp.zeros_like(below)

    c_in.wait()
    place = lax.broadcasted_iota(jnp.int32, (Z, L), 0)

    def step_row(t, y):
        now, later = t % 2, (t + 1) % 2
        if y == 0:
            arrived(lat.at[now], lat_recv.at[now])
        arrived(lon.at[now, y], lon_recv.at[now, y])
        arrived(lev.at[now, y], lev_recv.at[now, y])
        before, after = rows_beside(t, y)
        field[now, y, X] = lon[now, y, 1]

        def block(at, carry):
            left, middle = carry
            start = pl.multiple_of(at * BLOCK, BLOCK)
            for i in range(BLOCK):
                x = start + i
                right = field[now, y, x + 1]
                lower = jnp.where(place == 0, lev[now, y, 0, pl.ds(x, 1), :], pltpu.roll(middle, 1, 0))
                upper = jnp.where(place == Z - 1, lev[now, y, 1, pl.ds(x, 1), :], pltpu.roll(middle, Z - 1, 0))
                around = (left + right) + (before[x] + after[x]) + (lower + upper)
                new = 0.1 * around + middle * (0.6 - 0.2 * (middle * crowd[y, x]))
                field[later, y, x] = new
                face[t + 1, 0, y, pl.ds(x, 1), :] = new[0:1]
                face[t + 1, 1, y, pl.ds(x, 1), :] = new[Z - 1 : Z]
                left, middle = middle, right
            return left, middle

        lax.fori_loop(0, X // BLOCK, block, (lon[now, y, 0], field[now, y, 0]))

    def last_row(y):
        now = LAST % 2
        if y == 0:
            arrived(lat.at[now], lat_recv.at[now])
        arrived(lon.at[now, y], lon_recv.at[now, y])
        before, after = rows_beside(LAST, y)
        field[now, y, X] = lon[now, y, 1]

        def block(at, carry):
            left, middle = carry
            start = pl.multiple_of(at * BLOCK, BLOCK)
            for i in range(BLOCK):
                x = start + i
                right = field[now, y, x + 1]
                lower = jnp.where(place == 0, 0.0, pltpu.roll(middle, 1, 0))
                upper = jnp.where(place == Z - 1, 0.0, pltpu.roll(middle, Z - 1, 0))
                around = (left + right) + (before[x] + after[x]) + (lower + upper)
                new = 0.1 * around + middle * (0.6 - 0.2 * (middle * crowd[y, x]))
                end[y, x] = new
                shift = 1
                while shift < Z:
                    new = new + jnp.where(place >= shift, pltpu.roll(new, shift, 0), 0.0)
                    shift *= 2
                scan[y, x] = new
                sums[y, pl.ds(x, 1), :] = new[Z - 1 : Z]
                left, middle = middle, right
            return left, middle

        lax.fori_loop(0, X // BLOCK, block, (lon[now, y, 0], field[now, y, 0]))

    def sum_copy(y):
        return send(sums.at[y], below.at[y], sum_send, sum_recv.at[y], "lev", 1)

    def send_sum(y, wait):
        if wait:
            sum_copy(y).wait_recv()
        from_below = below[y] + upper_part * face[LAST, 0, y]
        sums[y] = (from_below + 0.1 * face[LAST, 1, y]) + sums[y]
        sum_copy(y).start()

    def last_down(y):
        return down(LAST, y, lev_recv.at[LAST % 2, y])

    def last_up(y):
        return up(LAST, y, lev_recv.at[LAST % 2, y])

    def send_top(y):
        send(face.at[LAST, 1, y], top.at[y], lev_send, top_recv.at[y], "lev", -1).start()

    def relay_top(y):
        copy = send(top.at[y], top.at[y], top_send, top_recv.at[y], "lev", -1)
        copy.wait_recv()
        copy.start()

    plans = [last_plan(k, levels, Y) for k in range(levels)]

    def act(k, kind, which):
        y = order[which]
        if kind == "sum":
            send_sum(y, True)
        elif kind == "up" and which >= Y - holds(k):
            @pl.when(~gives_way)
            def _():
                last_up(y).start()
        elif kind == "up":
            last_up(y).start()
        elif kind == "low":
            last_down(y).start()
        elif k == levels - 1:
            send_top(y)
        else:
            relay_top(y)

    for t in range(LAST):
        if t >= 1:
            plane_sent(t - 1)
        for at, y in enumerate(order):
            step_row(t, y)
            if t < LAST - 1:
                send_level(t + 1, y)
            send_plane(t + 1, y)
            if t < LAST - 1:
                continue

            for k in range(levels):
                if plans[k][0][at]:
                    @pl.when(level == k)
                    def _():
                        for kind, which in plans[k][0][at]:
                            act(k, kind, which)

            done = set(order[: at + 1])
            earlier = set(order[:at])
            ready = [
                row for row in order
                if {max(row - 1, 0), row, min(row + 1, Y - 1)} <= done
                and not {max(row - 1, 0), row, min(row + 1, Y - 1)} <= earlier
            ]
            for row in ready:
                last_row(row)

                @pl.when(level == 0)
                def _():
                    send_sum(row, False)

    for k in range(levels):
        @pl.when(level == k)
        def _():
            for kind, which in plans[k][1]:
                act(k, kind, which)

    now = LAST % 2
    for at, y in enumerate(order):
        @pl.when(level == levels - 1)
        def _():
            sum_copy(y).wait_recv()
            top[y] = face[LAST, 1, y]

        @pl.when(level == 0)
        def _():
            arrived(top.at[y], top_recv.at[y])
            lev[now, y, 0] = top[y]

        base[y] = (below[y] + upper_part * face[LAST, 0, y]) + 0.1 * top[y]

        @pl.when(level == 0)
        def _():
            last_down(y).wait_recv()

        @pl.when(level > 0)
        def _():
            arrived(lev.at[now, y], lev_recv.at[now, y])

        if at == max(Y - 3, 0):
            for k in range(levels - 1):
                @pl.when((level == k) & gives_way)
                def _():
                    for held in order[Y - holds(k) :]:
                        last_up(held).start()

        for start in range(0, X, PIECE):
            some = pl.ds(start, PIECE)
            upper = 0.1 * lev[now, y, 1, some, :]
            end[y, some, 0, :] = end[y, some, 0, :] + 0.1 * lev[now, y, 0, some, :]
            end[y, some, Z - 1, :] = end[y, some, Z - 1, :] + upper
            scan[y, some, Z - 1, :] = scan[y, some, Z - 1, :] + upper

    @pl.when(level < levels - 1)
    def _():
        arrived(sums, sum_send)

    @pl.when((level > 0) & (level < levels - 1))
    def _():
        arrived(top, top_send)

    arrived(face, lev_send)
    for t in (LAST - 1, LAST):
        plane_sent(t)


def finish(scale, end, scan, base, pot_hbm, end_hbm, pot, out_sem):
    Y, X, Z, L = pot.shape
    part = X // 4
    for y in range(Y):
        for x in range(0, X, part):
            some = pl.ds(x, part)
            pltpu.make_async_copy(end.at[y, some], end_hbm.at[y, some], out_sem.at[0]).start()
    for y in range(Y):
        @pl.loop(0, X // BLOCK)
        def _(at):
            start = pl.multiple_of(at * BLOCK, BLOCK)
            for i in range(BLOCK):
                x = start + i
                pot[y, x] = (scan[y, x] + base[y, pl.ds(x, 1), :]) * scale

        for x in range(0, X, part):
            some = pl.ds(x, part)
            pltpu.make_async_copy(pot.at[y, some], pot_hbm.at[y, some], out_sem.at[1]).start()
    pltpu.make_async_copy(end, end_hbm, out_sem.at[0]).wait()
    pltpu.make_async_copy(pot, pot_hbm, out_sem.at[1]).wait()


def per_device(sizes, field_values, crowding):
    Y, X, Z, L = field_values.shape
    f32 = jnp.float32
    dma = pltpu.SemaphoreType.DMA
    in_hbm = pl.BlockSpec(memory_space=pltpu.HBM)
    in_vmem = pl.BlockSpec(memory_space=pltpu.VMEM)
    shape = jax.ShapeDtypeStruct(field_values.shape, f32)
    end, scan, base = pl.pallas_call(
        functools.partial(march, sizes),
        out_shape=(pltpu.VMEM((Y, X, Z, L), f32), pltpu.VMEM((Y, X, Z, L), f32), pltpu.VMEM((Y, X, L), f32)),
        in_specs=[in_hbm, in_hbm],
        out_specs=(in_vmem, in_vmem, in_vmem),
        scratch_shapes=[
            pltpu.VMEM((2, Y, X + 1, Z, L), f32),
            pltpu.VMEM((Y, X, Z, L), f32),
            pltpu.VMEM((2, 2, X, Z, L), f32),
            pltpu.VMEM((2, Y, 2, Z, L), f32),
            pltpu.VMEM((2, Y, 2, X, L), f32),
            pltpu.VMEM((STEPS, 2, Y, X, L), f32),
            pltpu.VMEM((Y, X, L), f32),
            pltpu.VMEM((Y, X, L), f32),
            pltpu.VMEM((Y, X, L), f32),
            dma((2,)),
            dma((3,)),
            dma((2,)),
            dma((2,)),
            dma((2,)),
            dma((2, Y)),
            dma,
            dma((2, Y)),
            dma,
            dma((Y,)),
            dma,
            dma((Y,)),
            pltpu.SemaphoreType.REGULAR((2, 2)),
        ],
        compiler_params=pltpu.CompilerParams(
            collective_id=0, has_side_effects=True, vmem_limit_bytes=40 * 1024 * 1024
        ),
    )(field_values, crowding)
    return pl.pallas_call(
        functools.partial(finish, 1.0 / (Z * sizes["lev"])),
        out_shape=(shape, shape),
        in_specs=[in_vmem, in_vmem, in_vmem],
        out_specs=(in_hbm, in_hbm),
        scratch_shapes=[pltpu.VMEM((Y, X, Z, L), f32), dma((2,))],
        compiler_params=pltpu.CompilerParams(vmem_limit_bytes=12 * 1024 * 1024),
    )(end, scan, base)


def solution(mesh):
    return jax.shard_map(
        functools.partial(per_device, dict(mesh.shape)),
        mesh=mesh,
        in_specs=(P("lat", "lon", "lev", None), P("lat", "lon", "lev", None)),
        out_specs=(P("lat", "lon", "lev", None), P("lat", "lon", "lev", None)),
        check_vma=False,
    )
```
